128 devices in a mesh: row: 8 (over x, core), col: 16 (over z, y).
Axes of the slice: x: 4, y: 4, z: 4, core: 2. Of those that a mesh axis runs over, the one named last changes fastest.
Arguments:
- tail_vectors: float32 [64512, 4096], P('row', 'col'), may hold values from -6 to 6
- lower_panel: float32 [64512, 1024], P(('row', 'col')), may hold values from -0.0234375 to 0.0234375
- window_rhs: float32 [1024, 4096], P('row', 'col'), may hold values from -6 to 6
- window_block: float32 [1024, 1024], P(('row', 'col')), may hold values from -1 to 2, as said below
Outputs:
- window_vectors: float32 [1024, 4096], P('row', 'col')
The draws below stay inside these ranges and needn't reach their ends.
Inputs may be any that keep to these rules, and one draw needn't show every extreme that they name: window_block is zero above the diagonal; its diagonal lies in 1 to 2; entries below the diagonal are under 1 / sqrt(1024) in magnitude.
All inputs are finite; a program needn't handle non-finite values.
Results may differ from the reference program's by a relative error of at most 0.000082.
Values sent between devices are 32-bit elements; how exact they have to be, the bound alone decides.
A program may use at most 128 MiB of HBM per device.

```python
import jax
import jax.numpy as jnp
from jax import lax

NEV = 4096
WIN = 1024
TAIL = 64512


def draw_window_block(key, part):
    key_lower = jax.random.fold_in(key, 11)
    key_diag = jax.random.fold_in(key, 12)
    lower_mask = jnp.tril(jnp.ones((WIN, WIN), jnp.float32), -1)
    magnitude = 1.0 / jnp.sqrt(jnp.float32(WIN))
    spread = 0.98 * jax.random.uniform(key_lower, (WIN, WIN), jnp.float32, -1.0, 1.0)
    diagonal = jnp.exp(jax.random.uniform(key_diag, (WIN,), jnp.float32, 0.0, 0.69))
    return lower_mask * spread * magnitude + jnp.diag(diagonal)


def shard_levels(key, dims, cuts, smallest, high):
    factor_of, own = 1.0, jax.random.fold_in(key, 6)
    for position, parts in cuts:
        steps = jnp.exp(jax.random.uniform(jax.random.fold_in(own, position), (parts,), jnp.float32, smallest / len(cuts), high / len(cuts)))
        factor_of = factor_of * jnp.repeat(steps, dims[position] // parts).reshape([-1 if axis == position else 1 for axis in range(len(dims))])
    return factor_of


def centred(own_key, extent, scale, limit, shards=(), kind=jnp.bfloat16):
    drawn = jax.random.normal(own_key, extent, jnp.float32) * scale
    if len(shards) > 0:
        drawn = shard_levels(own_key, extent, shards, -0.22, 0.18) * drawn
    return jnp.clip(drawn, min=-limit, max=limit).astype(kind)


def setup_inputs(seed: int = 0) -> dict:
    key_list = jax.random.split(jax.random.key(seed), 5)
    return {
        "tail_vectors": centred(key_list[0], (TAIL, NEV), 1.0, 6.0, ((0, 8), (1, 16)), jnp.float32),
        "lower_panel": centred(key_list[1], (TAIL, WIN), TAIL ** -0.5, 0.0234375, ((0, 128),), jnp.float32),
        "window_rhs": centred(key_list[2], (WIN, NEV), 1.0, 6.0, ((0, 8), (1, 16)), jnp.float32),
        "window_block": draw_window_block(jax.random.fold_in(key_list[4], 71), 0),
    }


def reference(tail_vectors, lower_panel, window_rhs, window_block):
    correction = lax.dot_general(lower_panel.astype(jnp.float32), tail_vectors.astype(jnp.float32), (((0,), (0,)), ((), ())), precision=lax.Precision.HIGHEST, preferred_element_type=jnp.float32)
    right_side = window_rhs - correction
    return jax.scipy.linalg.solve_triangular(window_block, right_side, trans=1, lower=True)
```

```python
import functools

import jax
import jax.numpy as jnp
from jax import lax
from jax.experimental import pallas as pl
from jax.experimental.pallas import tpu as pltpu
from jax.sharding import PartitionSpec as P

F32, BF16 = jnp.float32, jnp.bfloat16
HIGHEST = lax.Precision.HIGHEST
SEG = 504
PAD = 512
WIN = 1024
COLS = 256
BLK = 128


def split(value):
    high = value.astype(BF16)
    return high, (value - high.astype(F32)).astype(BF16)


def dot(a, b, precision=None):
    return jnp.dot(a, b, preferred_element_type=F32, precision=precision)


def kernel(
    tail, panel, rhs, block, out,
    tbuf, fwd, lbuf, lsplit, tt, acc, wrow, gfull, gsplit, rhs_in,
    r1, part, ring1, ring2, psum, r3, xs, obuf,
    send_sem, recv_sem, local_sem,
):
    row, col = lax.axis_index("row"), lax.axis_index("col")
    x, core = row // 2, row % 2
    z, y = col // 4, col % 4
    counter = [0]
    started = []

    def where(dx=0, dc=0, dz=0, dy=0):
        new_row = 2 * ((x + dx + 4) % 4) + (core + dc) % 2
        new_col = 4 * ((z + dz + 4) % 4) + (y + dy + 4) % 4
        return (new_row, new_col)

    def copy(src, dst, target):
        index = counter[0]
        counter[0] += 1
        made = pltpu.make_async_remote_copy(
            src_ref=src,
            dst_ref=dst,
            send_sem=send_sem.at[index],
            recv_sem=recv_sem.at[index],
            device_id=target,
            device_id_type=pl.DeviceIdType.MESH,
        )
        made.start()
        started.append(made)
        return made

    def tail_rows(e, dy):
        start = (4 * ((z - e + 4) % 4) + (y + dy + 4) % 4) * SEG
        return tail.at[pl.ds(pl.multiple_of(start, 8), SEG), :]

    partners = [where(dy=i) for i in (1, 2, 3)] + [where(dz=i) for i in (1, 2, 3)]
    partners += [where(dx=i, dc=j) for i in range(4) for j in range(2) if (i, j) != (0, 0)]
    barrier = pltpu.get_barrier_semaphore()
    for partner in partners:
        pl.semaphore_signal(barrier, inc=1, device_id=partner, device_id_type=pl.DeviceIdType.MESH)
    pl.semaphore_wait(barrier, len(partners))

    mine = pl.ds(pl.multiple_of(col * 8, 8), 8)
    over_y = [copy(block, wrow.at[mine, :], where(dy=i)) for i in (1, 3, 2)]

    far_up = [copy(tail_rows(e, 2), fwd.at[i], where(dy=1)) for i, e in enumerate((0, 1))]
    far_down = [copy(tail_rows(e, 2), fwd.at[2 + i], where(dy=3)) for i, e in enumerate((3, 2))]
    near_up, near_down = {}, {}
    for e in (0, 1, 3, 2):
        near_up[e] = copy(tail_rows(e, 1), tbuf.at[1, e, pl.ds(0, SEG), :], where(dy=1))
        near_down[e] = copy(tail_rows(e, 3), tbuf.at[3, e, pl.ds(0, SEG), :], where(dy=3))

    local = []

    def bring(src, dst):
        made = pltpu.make_async_copy(src, dst, local_sem.at[len(local)])
        made.start()
        local.append(made)
        return made

    own_block = bring(block, wrow.at[mine, :])
    own_panel = bring(panel, lbuf.at[0, pl.ds(0, SEG), :])
    own_rhs = bring(rhs, rhs_in)
    own_tail = {e: bring(tail_rows(e, 0), tbuf.at[0, e, pl.ds(0, SEG), :]) for e in range(4)}

    for e in range(4):
        lbuf[e, SEG:, :] = jnp.zeros((PAD - SEG, WIN), F32)
        for d in range(4):
            tbuf[d, e, SEG:, :] = jnp.zeros((PAD - SEG, COLS), F32)

    own_block.wait()
    for made in over_y:
        made.wait_recv()
    quarter = pl.ds(pl.multiple_of(z * 32, 32), 32)
    over_z = [copy(wrow.at[quarter, :], wrow.at[quarter, :], where(dz=i)) for i in (1, 3, 2)]

    top, bottom = pl.ds(0, 256), pl.ds(256, SEG - 256)
    up_first = copy(panel.at[top, :], lbuf.at[1, top, :], where(dz=1))
    down_first = copy(panel.at[bottom, :], lbuf.at[3, bottom, :], where(dz=3))
    up_second = copy(panel.at[bottom, :], lbuf.at[1, bottom, :], where(dz=1))
    down_second = copy(panel.at[top, :], lbuf.at[3, top, :], where(dz=3))

    for made in over_z:
        made.wait_recv()

    rows = lax.broadcasted_iota(jnp.int32, (BLK, BLK), 0)
    cols = lax.broadcasted_iota(jnp.int32, (BLK, BLK), 1)
    eye = jnp.where(rows == cols, 1.0, 0.0).astype(F32)
    own_cols = pl.ds(pl.multiple_of(row * BLK, BLK), BLK)
    diagonal = wrow[:, own_cols]
    on_diag = jnp.where(rows == cols, diagonal, 0.0)
    diag_rows = jnp.sum(on_diag, axis=1, keepdims=True)
    diag_cols = jnp.sum(on_diag, axis=0, keepdims=True)
    lower = jnp.where(rows > cols, diagonal, 0.0) / diag_rows

    inverse, power = eye - lower, dot(lower, lower, HIGHEST)
    for _ in range(6):
        both = dot(jnp.concatenate([inverse, power], axis=0), power, HIGHEST)
        inverse, power = inverse + both[:BLK], both[BLK:]
    inverse = inverse / diag_cols
    gfull[row] = dot(inverse, wrow[...], HIGHEST)
    gfull[row, :, own_cols] = inverse
    over_x = [copy(gfull.at[row], gfull.at[row], where(dx=i)) for i in (1, 3, 2)]
    across = [copy(gfull.at[row], gfull.at[row], where(dc=1))]

    def split_panel(e):
        @pl.loop(0, 4)
        def _(step):
            at = pl.ds(pl.multiple_of(step * BLK, BLK), BLK)
            high, low = split(lbuf[e, at, :])
            lsplit[e, pl.ds(pl.multiple_of(step * BLK, BLK), BLK), :] = low
            lsplit[e, pl.ds(pl.multiple_of(PAD + step * BLK, BLK), BLK), :] = high

    def product(d, e, first):
        @pl.loop(0, 4)
        def _(step):
            base = pl.multiple_of(step * BLK, BLK)
            high, low = split(tbuf[d, e, pl.ds(base, BLK), :].T)
            tt[:, pl.ds(base, BLK)] = high
            tt[:, pl.ds(pl.multiple_of(PAD + step * BLK, BLK), BLK)] = low

        @pl.loop(0, 4)
        def _(step):
            at = pl.ds(pl.multiple_of(step * 256, 256), 256)
            value = dot(tt[...], lsplit[e, :, at]) + dot(tt[:, :PAD], lsplit[e, PAD:, at])
            if first:
                acc[d, :, at] = value
            else:
                acc[d, :, at] += value

    own_panel.wait()
    split_panel(0)
    own_tail[0].wait()
    product(0, 0, True)
    own_rhs.wait()
    acc[0, :, own_cols] += -rhs_in[...].T

    far = {}
    for i, e in enumerate((0, 1)):
        far_up[i].wait_recv()
        far[e] = copy(fwd.at[i], tbuf.at[2, e, pl.ds(0, SEG), :], where(dy=1))
    for i, e in enumerate((3, 2)):
        far_down[i].wait_recv()
        far[e] = copy(fwd.at[2 + i], tbuf.at[2, e, pl.ds(0, SEG), :], where(dy=3))
    up_first.wait_recv()
    up_on = copy(lbuf.at[1, top, :], lbuf.at[2, top, :], where(dz=1))
    down_first.wait_recv()
    down_on = copy(lbuf.at[3, bottom, :], lbuf.at[2, bottom, :], where(dz=3))

    for made, i in zip(over_x, (1, 3, 2)):
        made.wait_recv()
        slot = 2 * ((x - i + 4) % 4) + core
        across.append(copy(gfull.at[slot], gfull.at[slot], where(dc=1)))

    near_up[0].wait_recv()
    product(1, 0, True)
    near_down[0].wait_recv()
    product(3, 0, True)

    for made in across:
        made.wait_recv()

    @pl.loop(0, 8)
    def _(step):
        high, low = split(gfull[step])
        gsplit[0, step] = high
        gsplit[1, step] = low

    for e in (1, 3):
        own_tail[e].wait()
    up_second.wait_recv()
    split_panel(1)
    product(0, 1, False)
    down_second.wait_recv()
    split_panel(3)
    product(0, 3, False)
    for e in (1, 3):
        near_up[e].wait_recv()
        product(1, e, False)
        near_down[e].wait_recv()
        product(3, e, False)

    up_on.wait_recv()
    down_on.wait_recv()
    split_panel(2)

    pair, first_hop, second_hop, third = {}, {}, {}, {}
    keep = pl.ds(pl.multiple_of(core * BLK, BLK), BLK)
    give = pl.ds(pl.multiple_of((1 - core) * BLK, BLK), BLK)
    upper, under = pl.ds(0, 16), pl.ds(16, 16)
    x_up, x_down, x_far = (x + 1) % 4, (x + 3) % 4, (x + 2) % 4

    def to_pair(d):
        pair[d] = copy(acc.at[d, give, :], r1.at[d], where(dc=1))

    def to_ring(d):
        pair[d].wait_recv()
        part[d] = (acc[d, keep, :] + r1[d]).reshape(4, 32, WIN)
        first_hop[d] = (
            copy(part.at[d, x_far, upper, :], ring1.at[d, 0], where(dx=1)),
            copy(part.at[d, x_far, under, :], ring1.at[d, 1], where(dx=3)),
        )

    def round_ring(d):
        first_hop[d][0].wait_recv()
        part[d, x_up, upper, :] += ring1[d, 0]
        up = copy(part.at[d, x_up], ring2.at[d, 0], where(dx=1))
        first_hop[d][1].wait_recv()
        part[d, x_down, under, :] += ring1[d, 1]
        second_hop[d] = (up, copy(part.at[d, x_down], ring2.at[d, 1], where(dx=3)))

    def from_ring(d):
        second_hop[d][0].wait_recv()
        second_hop[d][1].wait_recv()
        psum[d] = part[d, x] + ring2[d, 0] + ring2[d, 1]
        if d:
            third[d] = copy(psum.at[d], r3.at[d], where(dy=-d))

    own_tail[2].wait()
    product(0, 2, False)
    to_pair(0)
    near_up[2].wait_recv()
    product(1, 2, False)
    to_pair(1)
    to_ring(0)
    near_down[2].wait_recv()
    product(3, 2, False)
    to_pair(3)
    to_ring(1)
    to_ring(3)
    far[0].wait_recv()
    product(2, 0, True)
    for d in (0, 1, 3):
        round_ring(d)
    far[3].wait_recv()
    product(2, 3, False)
    for d in (0, 1, 3):
        from_ring(d)
    for e in (1, 2):
        far[e].wait_recv()
        product(2, e, False)
    to_pair(2)
    to_ring(2)
    round_ring(2)
    from_ring(2)

    total = psum[0]
    for d in (1, 3, 2):
        third[d].wait_recv()
        total += r3[d]

    left = -total
    for j in range(7, -1, -1):
        high, low = split(left[:, j * BLK : (j + 1) * BLK])
        width = (j + 1) * BLK
        both = dot(jnp.concatenate([high, low], axis=0), gsplit[0, j, :, :width])
        step = both[:32] + both[32:] + dot(high, gsplit[1, j, :, :width])
        xs[j] = step[:, j * BLK :]
        if j:
            left = left[:, : j * BLK] - step[:, : j * BLK]

    own = pl.ds(pl.multiple_of(core * BLK + x * 32, 32), 32)
    obuf[own, :] = xs[row]
    spread = []
    for i in range(4):
        for j in range(2):
            if (i, j) != (0, 0):
                target = where(dx=i, dc=j)
                spread.append(copy(xs.at[target[0]], obuf.at[own, :], target))
    for made in spread:
        made.wait_recv()
    out[...] = obuf[...].T
    for made in started:
        made.wait_send()


COPIES = 80


def per_device(tail_vectors, lower_panel, window_rhs, window_block):
    anywhere = pl.BlockSpec(memory_space=pl.ANY)
    return pl.pallas_call(
        kernel,
        name="window_solve",
        out_shape=jax.ShapeDtypeStruct((BLK, COLS), F32),
        in_specs=[anywhere] * 4,
        out_specs=pl.BlockSpec(memory_space=pltpu.VMEM),
        scratch_shapes=[
            pltpu.VMEM((4, 4, PAD, COLS), F32),
            pltpu.VMEM((4, SEG, COLS), F32),
            pltpu.VMEM((4, PAD, WIN), F32),
            pltpu.VMEM((4, 2 * PAD, WIN), BF16),
            pltpu.VMEM((COLS, 2 * PAD), BF16),
            pltpu.VMEM((4, COLS, WIN), F32),
            pltpu.VMEM((BLK, WIN), F32),
            pltpu.VMEM((8, BLK, WIN), F32),
            pltpu.VMEM((2, 8, BLK, WIN), BF16),
            pltpu.VMEM((BLK, COLS), F32),
            pltpu.VMEM((4, BLK, WIN), F32),
            pltpu.VMEM((4, 4, 32, WIN), F32),
            pltpu.VMEM((4, 2, 16, WIN), F32),
            pltpu.VMEM((4, 2, 32, WIN), F32),
            pltpu.VMEM((4, 32, WIN), F32),
            pltpu.VMEM((4, 32, WIN), F32),
            pltpu.VMEM((8, 32, BLK), F32),
            pltpu.VMEM((COLS, BLK), F32),
            pltpu.SemaphoreType.DMA((COPIES,)),
            pltpu.SemaphoreType.DMA((COPIES,)),
            pltpu.SemaphoreType.DMA((8,)),
        ],
        compiler_params=pltpu.CompilerParams(
            collective_id=0, has_side_effects=True, vmem_limit_bytes=62 * 1024 * 1024
        ),
    )(tail_vectors, lower_panel, window_rhs, window_block)


def solution(mesh):
    in_specs = (P("row", "col"), P(("row", "col"), None), P("row", "col"), P(("row", "col"), None))
    return jax.shard_map(
        per_device, mesh=mesh, in_specs=in_specs, out_specs=P("row", "col"), check_vma=False
    )
```

```python
import jax
import jax.numpy as jnp
from jax import lax
from jax.experimental import pallas as pl
from jax.experimental.pallas import tpu as pltpu
from jax.sharding import PartitionSpec as P

F32, BF16 = jnp.float32, jnp.bfloat16
HIGHEST = lax.Precision.HIGHEST
SEG = 504
LEN = (256, 248)
PART = 256
DEEP = 4 * PART
WIN = 1024
COLS = 256
BLK = 128
QUARTER = 16
CHUNKS = [(None, 0, 0), (None, 0, 1)] + [(p, d, h) for h in range(2) for d in (1, 3, 2) for p in range(2)]
NUMBER = {chunk: q for q, chunk in enumerate(CHUNKS)}
COPIES = 112


def split(value):
    high = value.astype(BF16)
    return high, (value - high.astype(F32)).astype(BF16)


def dot(a, b, precision=None):
    return jnp.dot(a, b, preferred_element_type=F32, precision=precision)


def aligned(start, size, unit):
    return pl.ds(pl.multiple_of(start, unit), size)


def kernel(
    tail, panel, rhs, block, out,
    tbuf, lbuf, lsplit, tt, cbuf, wrow, gfull, gsplit, rhs_in,
    r1, part, ring, psum, r3, xs, obuf,
    send_sem, recv_sem, local_sem,
):
    row, col = lax.axis_index("row"), lax.axis_index("col")
    x, core = row // 2, row % 2
    z, y = col // 4, col % 4
    counter = [0]
    started = []

    def where(dx=0, dc=0, dz=0, dy=0):
        new_row = 2 * ((x + dx + 4) % 4) + (core + dc) % 2
        new_col = 4 * ((z + dz + 4) % 4) + (y + dy + 4) % 4
        return (new_row, new_col)

    def along(p, step):
        return where(dy=step) if p == 0 else where(dz=step)

    def across(p, step):
        return along(1 - p, step)

    place = (z, y)

    def copy(src, dst, target):
        index = counter[0]
        counter[0] += 1
        made = pltpu.make_async_remote_copy(
            src_ref=src,
            dst_ref=dst,
            send_sem=send_sem.at[index],
            recv_sem=recv_sem.at[index],
            device_id=target,
            device_id_type=pl.DeviceIdType.MESH,
        )
        made.start()
        started.append(made)
        return made

    local = []

    def bring(src, dst):
        made = pltpu.make_async_copy(src, dst, local_sem.at[len(local)])
        made.start()
        local.append(made)
        return made

    def piece(p, step, h):
        columns = pl.ds(h * BLK, BLK)
        if p == 0:
            return tail.at[:, (y + step) % 4, pl.ds(0, LEN[0]), columns]
        return tail.at[(z + step) % 4, :, pl.ds(LEN[0], LEN[1]), columns]

    def landing(p, d, h):
        return tbuf.at[p, d, h, :, pl.ds(0, LEN[p]), :]

    partners = [where(dy=i) for i in (1, 2, 3)] + [where(dz=i) for i in (1, 2, 3)]
    partners += [where(dx=i, dc=j) for i in range(4) for j in range(2) if (i, j) != (0, 0)]
    barrier = pltpu.get_barrier_semaphore()
    for partner in partners:
        pl.semaphore_signal(barrier, inc=1, device_id=partner, device_id_type=pl.DeviceIdType.MESH)
    pl.semaphore_wait(barrier, len(partners))

    mine = aligned(col * 8, 8, 8)
    over_y = [copy(block, wrow.at[mine, :], where(dy=i)) for i in (1, 3, 2)]

    def half(p, side):
        return pl.ds(0, 128) if side == 0 else pl.ds(128, LEN[p] - 128)

    def send_panel(p, step, side):
        src = pl.ds(p * PART + half(p, side).start, half(p, side).size)
        return copy(panel.at[src, :], lbuf.at[p, place[p], half(p, side), :], across(p, step))

    first = [(send_panel(p, 1, 0), send_panel(p, 3, 1)) for p in (1, 0)]
    own_block = bring(block, wrow.at[mine, :])
    own_panel = [
        bring(panel.at[pl.ds(p * PART, LEN[p]), :], lbuf.at[p, place[p], pl.ds(0, LEN[p]), :]) for p in range(2)
    ]
    own_rhs = bring(rhs, rhs_in)
    own_tail = [bring(piece(p, 0, h), landing(p, 0, h)) for p in range(2) for h in range(2)]
    second = [(send_panel(1, 1, 1), send_panel(1, 3, 0))]

    for i in range(4):
        lbuf[1, i, LEN[1] :, :] = jnp.zeros((PART - LEN[1], WIN), F32)
        for d in range(4):
            for h in range(2):
                tbuf[1, d, h, i, LEN[1] :, :] = jnp.zeros((PART - LEN[1], BLK), F32)

    own_block.wait()
    for made in over_y:
        made.wait_recv()
    quarter = aligned(z * 32, 32, 32)
    over_z = [copy(wrow.at[quarter, :], wrow.at[quarter, :], where(dz=i)) for i in (1, 3, 2)]
    second.append((send_panel(0, 1, 1), send_panel(0, 3, 0)))

    onward = []
    for p, (up, down) in zip((1, 0), first):
        below, above = (place[p] + 3) % 4, (place[p] + 1) % 4
        up.wait_recv()
        at = lbuf.at[p, below, half(p, 0), :]
        onward.append(copy(at, at, across(p, 1)))
        down.wait_recv()
        at = lbuf.at[p, above, half(p, 1), :]
        onward.append(copy(at, at, across(p, 3)))

    pieces = {}
    for h in range(2):
        for d in (1, 3, 2):
            for p in range(2):
                pieces[p, d, h] = copy(piece(p, d, h), landing(p, d, h), along(p, d))

    for made in over_z:
        made.wait_recv()

    rows = lax.broadcasted_iota(jnp.int32, (BLK, BLK), 0)
    cols = lax.broadcasted_iota(jnp.int32, (BLK, BLK), 1)
    eye = jnp.where(rows == cols, 1.0, 0.0).astype(F32)
    own_cols = aligned(row * BLK, BLK, BLK)
    diagonal = wrow[:, own_cols]
    on_diag = jnp.where(rows == cols, diagonal, 0.0)
    diag_rows = jnp.sum(on_diag, axis=1, keepdims=True)
    diag_cols = jnp.sum(on_diag, axis=0, keepdims=True)
    lower = jnp.where(rows > cols, diagonal, 0.0) / diag_rows
    inverse, power = eye - lower, dot(lower, lower, HIGHEST)
    for _ in range(6):
        both = dot(jnp.concatenate([inverse, power], axis=0), power, HIGHEST)
        inverse, power = inverse + both[:BLK], both[BLK:]
    inverse = inverse / diag_cols
    gfull[row] = dot(inverse, wrow[...], HIGHEST)
    gfull[row, :, own_cols] = inverse
    over_x = [copy(gfull.at[row], gfull.at[row], where(dx=i)) for i in (1, 3, 2)]
    to_other = [copy(gfull.at[row], gfull.at[row], where(dc=1))]

    for made in own_panel:
        made.wait()
    for up, down in second:
        up.wait_recv()
        down.wait_recv()
    for made in onward:
        made.wait_recv()

    @pl.loop(0, 2)
    def _(p):
        @pl.loop(0, 8)
        def _(step):
            high, low = split(lbuf[p, step // 2, aligned((step % 2) * BLK, BLK, BLK), :])
            lsplit[p, aligned(step * BLK, BLK, BLK), :] = low
            lsplit[p, aligned(DEEP + step * BLK, BLK, BLK), :] = high

    def product(p, sources, store):
        for i, (d, h) in enumerate(sources):

            @pl.loop(0, 4)
            def _(step):
                high, low = split(tbuf[p, d, h, step].T)
                tt[pl.ds(i * BLK, BLK), aligned(step * PART, PART, PART)] = high
                tt[pl.ds(i * BLK, BLK), aligned(DEEP + step * PART, PART, PART)] = low

        height = pl.ds(0, len(sources) * BLK)

        @pl.loop(0, 4)
        def _(step):
            at = aligned(step * 256, 256, 256)
            value = dot(tt[height, :], lsplit[p, :, at]) + dot(tt[height, :DEEP], lsplit[p, DEEP:, at])
            for i in range(len(sources)):
                store(i, at, value[i * BLK : (i + 1) * BLK])

    keep, give = aligned(core * 64, 64, 64), aligned((1 - core) * 64, 64, 64)
    pair, ringed, third = {}, {}, {}

    def to_pair(q):
        pair[q] = copy(cbuf.at[q, give, :], r1.at[q], where(dc=1))

    def to_ring(q):
        pair[q].wait_recv()
        part[q] = (cbuf[q, keep, :] + r1[q]).reshape(4, QUARTER, WIN)
        ringed[q] = [copy(part.at[q, (x + i) % 4], ring.at[q, i - 1], where(dx=i)) for i in (2, 1, 3)]

    def from_ring(q):
        for made in ringed[q]:
            made.wait_recv()
        psum[q] = part[q, x] + ring[q, 0] + ring[q, 1] + ring[q, 2]
        p, d, _ = CHUNKS[q]
        if d:
            third[q] = copy(psum.at[q], r3.at[q - 2], along(p, -d))

    def chunk_product(p, sources):
        numbers = [NUMBER[p, d, h] for d, h in sources]
        for d, h in sources:
            pieces[p, d, h].wait_recv()

        def store(i, at, value):
            cbuf[numbers[i], :, at] = value

        product(p, sources, store)
        for q in numbers:
            to_pair(q)
        return numbers

    def store_own(i, at, value):
        cbuf[i, :, at] = value

    def add_own(i, at, value):
        cbuf[i, :, at] += value

    for made in own_tail:
        made.wait()
    product(0, [(0, 0), (0, 1)], store_own)
    product(1, [(0, 0), (0, 1)], add_own)
    own_rhs.wait()
    turned = rhs_in[...].T
    for h in range(2):
        cbuf[h, :, own_cols] += -turned[h * BLK : (h + 1) * BLK]
        to_pair(h)
    for made, i in zip(over_x, (1, 3, 2)):
        made.wait_recv()
        slot = 2 * ((x - i + 4) % 4) + core
        to_other.append(copy(gfull.at[slot], gfull.at[slot], where(dc=1)))
    to_ring(0)
    to_ring(1)

    a = chunk_product(0, [(1, 0), (3, 0)])
    b = chunk_product(1, [(1, 0), (3, 0)])
    for q in a + b:
        to_ring(q)

    for made in to_other:
        made.wait_recv()

    @pl.loop(0, 8)
    def _(step):
        high, low = split(gfull[step])
        gsplit[0, step] = high
        gsplit[1, step] = low

    from_ring(0)
    from_ring(1)
    c = chunk_product(0, [(2, 0)]) + chunk_product(1, [(2, 0)])
    for q in a + b:
        from_ring(q)
    for q in c:
        to_ring(q)
    a = chunk_product(0, [(1, 1), (3, 1)])
    b = chunk_product(1, [(1, 1), (3, 1)])
    for q in c:
        from_ring(q)
    for q in a + b:
        to_ring(q)
    c = chunk_product(0, [(2, 1)])
    for q in a + b:
        from_ring(q)
    c += chunk_product(1, [(2, 1)])
    for q in c:
        to_ring(q)
    totals = []
    for h in range(2):
        if h:
            for q in c:
                from_ring(q)
        total = psum[h]
        for d in (1, 3, 2):
            for p in range(2):
                q = NUMBER[p, d, h]
                third[q].wait_recv()
                total += r3[q - 2]
        totals.append(total)

    left = -jnp.concatenate(totals, axis=0)
    for j in range(7, -1, -1):
        high, low = split(left[:, j * BLK : (j + 1) * BLK])
        width = (j + 1) * BLK
        both = dot(jnp.concatenate([high, low], axis=0), gsplit[0, j, :, :width])
        step = both[:32] + both[32:] + dot(high, gsplit[1, j, :, :width])
        xs[j] = step[:, j * BLK :].reshape(2, QUARTER, BLK)
        if j:
            left = left[:, : j * BLK] - step[:, : j * BLK]

    own = aligned(core * 64 + x * QUARTER, QUARTER, QUARTER)
    obuf[:, own, :] = xs[row]
    spread = []
    for i in range(4):
        for j in range(2):
            if (i, j) != (0, 0):
                target = where(dx=i, dc=j)
                spread.append(copy(xs.at[target[0]], obuf.at[:, own, :], target))
    for made in spread:
        made.wait_recv()
    out[...] = obuf[...].reshape(COLS, BLK).T
    for made in started:
        made.wait_send()


def per_device(tail_vectors, lower_panel, window_rhs, window_block):
    anywhere = pl.BlockSpec(memory_space=pl.ANY)
    count = len(CHUNKS)
    return pl.pallas_call(
        kernel,
        name="window_solve",
        out_shape=jax.ShapeDtypeStruct((BLK, COLS), F32),
        in_specs=[anywhere] * 4,
        out_specs=pl.BlockSpec(memory_space=pltpu.VMEM),
        scratch_shapes=[
            pltpu.VMEM((2, 4, 2, 4, PART, BLK), F32),
            pltpu.VMEM((2, 4, PART, WIN), F32),
            pltpu.VMEM((2, 2 * DEEP, WIN), BF16),
            pltpu.VMEM((COLS, 2 * DEEP), BF16),
            pltpu.VMEM((count, BLK, WIN), F32),
            pltpu.VMEM((BLK, WIN), F32),
            pltpu.VMEM((8, BLK, WIN), F32),
            pltpu.VMEM((2, 8, BLK, WIN), BF16),
            pltpu.VMEM((BLK, COLS), F32),
            pltpu.VMEM((count, 64, WIN), F32),
            pltpu.VMEM((count, 4, QUARTER, WIN), F32),
            pltpu.VMEM((count, 3, QUARTER, WIN), F32),
            pltpu.VMEM((count, QUARTER, WIN), F32),
            pltpu.VMEM((count - 2, QUARTER, WIN), F32),
            pltpu.VMEM((8, 2, QUARTER, BLK), F32),
            pltpu.VMEM((2, BLK, BLK), F32),
            pltpu.SemaphoreType.DMA((COPIES,)),
            pltpu.SemaphoreType.DMA((COPIES,)),
            pltpu.SemaphoreType.DMA((8,)),
        ],
        compiler_params=pltpu.CompilerParams(
            collective_id=0, has_side_effects=True, vmem_limit_bytes=62 * 1024 * 1024
        ),
    )(tail_vectors.reshape(4, 4, SEG, COLS), lower_panel, window_rhs, window_block)


def solution(mesh):
    in_specs = (P("row", "col"), P(("row", "col"), None), P("row", "col"), P(("row", "col"), None))
    return jax.shard_map(
        per_device, mesh=mesh, in_specs=in_specs, out_specs=P("row", "col"), check_vma=False
    )
```

```python
import jax
import jax.numpy as jnp
from jax import lax
from jax.experimental import pallas as pl
from jax.experimental.pallas import tpu as pltpu
from jax.sharding import PartitionSpec as P

F32, BF16 = jnp.float32, jnp.bfloat16
HIGHEST = lax.Precision.HIGHEST
SEG = 504
LEN = (256, 248)
PART = 256
DEEP = 4 * PART
WIN = 1024
COLS = 256
BLK = 128
QUARTER = 16
CHUNKS = [(None, 0, 0), (None, 0, 1)] + [(p, d, h) for near in ((1, 3), (2,)) for h in range(2) for d in near for p in range(2)]
NUMBER = {chunk: q for q, chunk in enumerate(CHUNKS)}
COPIES = 128


def split(value):
    high = value.astype(BF16)
    return high, (value - high.astype(F32)).astype(BF16)


def dot(a, b, precision=None):
    return jnp.dot(a, b, preferred_element_type=F32, precision=precision)


def aligned(start, size, unit):
    return pl.ds(pl.multiple_of(start, unit), size)


def kernel(
    tail, panel, rhs, block, out,
    tbuf, fwd, lbuf, lsplit, tt, cbuf, wrow, gfull, gsplit, rhs_in,
    r1, part, ring, psum, r3, xs, obuf,
    send_sem, recv_sem, local_sem,
):
    row, col = lax.axis_index("row"), lax.axis_index("col")
    x, core = row // 2, row % 2
    z, y = col // 4, col % 4
    counter = [0]
    started = []

    def where(dx=0, dc=0, dz=0, dy=0):
        new_row = 2 * ((x + dx + 4) % 4) + (core + dc) % 2
        new_col = 4 * ((z + dz + 4) % 4) + (y + dy + 4) % 4
        return (new_row, new_col)

    def along(p, step):
        return where(dy=step) if p == 0 else where(dz=step)

    def across(p, step):
        return along(1 - p, step)

    place = (z, y)

    def copy(src, dst, target):
        index = counter[0]
        counter[0] += 1
        made = pltpu.make_async_remote_copy(
            src_ref=src,
            dst_ref=dst,
            send_sem=send_sem.at[index],
            recv_sem=recv_sem.at[index],
            device_id=target,
            device_id_type=pl.DeviceIdType.MESH,
        )
        made.start()
        started.append(made)
        return made

    local = []

    def bring(src, dst):
        made = pltpu.make_async_copy(src, dst, local_sem.at[len(local)])
        made.start()
        local.append(made)
        return made

    def piece(p, step, h):
        columns = pl.ds(h * BLK, BLK)
        if p == 0:
            return tail.at[:, (y + step) % 4, pl.ds(0, LEN[0]), columns]
        return tail.at[(z + step) % 4, :, pl.ds(LEN[0], LEN[1]), columns]

    def landing(p, d, h):
        return tbuf.at[p, d, h, :, pl.ds(0, LEN[p]), :]

    partners = [where(dy=i) for i in (1, 2, 3)] + [where(dz=i) for i in (1, 2, 3)]
    partners += [where(dx=i, dc=j) for i in range(4) for j in range(2) if (i, j) != (0, 0)]
    barrier = pltpu.get_barrier_semaphore()
    for partner in partners:
        pl.semaphore_signal(barrier, inc=1, device_id=partner, device_id_type=pl.DeviceIdType.MESH)
    pl.semaphore_wait(barrier, len(partners))

    mine = aligned(col * 8, 8, 8)
    over_y = [copy(block, wrow.at[mine, :], where(dy=i)) for i in (1, 3, 2)]

    def half(p, side):
        return pl.ds(0, 128) if side == 0 else pl.ds(128, LEN[p] - 128)

    def send_panel(p, step, side):
        src = pl.ds(p * PART + half(p, side).start, half(p, side).size)
        return copy(panel.at[src, :], lbuf.at[p, place[p], half(p, side), :], across(p, step))

    first = [(send_panel(p, 1, 0), send_panel(p, 3, 1)) for p in (1, 0)]
    own_block = bring(block, wrow.at[mine, :])
    own_panel = [
        bring(panel.at[pl.ds(p * PART, LEN[p]), :], lbuf.at[p, place[p], pl.ds(0, LEN[p]), :]) for p in range(2)
    ]
    own_rhs = bring(rhs, rhs_in)
    own_tail = [bring(piece(p, 0, h), landing(p, 0, h)) for p in range(2) for h in range(2)]
    second = [(send_panel(1, 1, 1), send_panel(1, 3, 0))]

    for i in range(4):
        lbuf[1, i, LEN[1] :, :] = jnp.zeros((PART - LEN[1], WIN), F32)
        for d in range(4):
            for h in range(2):
                tbuf[1, d, h, i, LEN[1] :, :] = jnp.zeros((PART - LEN[1], BLK), F32)

    own_block.wait()
    for made in over_y:
        made.wait_recv()
    quarter = aligned(z * 32, 32, 32)
    over_z = [copy(wrow.at[quarter, :], wrow.at[quarter, :], where(dz=i)) for i in (1, 3, 2)]
    second.append((send_panel(0, 1, 1), send_panel(0, 3, 0)))

    onward = []
    for p, (up, down) in zip((1, 0), first):
        below, above = (place[p] + 3) % 4, (place[p] + 1) % 4
        up.wait_recv()
        at = lbuf.at[p, below, half(p, 0), :]
        onward.append(copy(at, at, across(p, 1)))
        down.wait_recv()
        at = lbuf.at[p, above, half(p, 1), :]
        onward.append(copy(at, at, across(p, 3)))

    pieces, hops, far = {}, {}, {}
    for p, d, h in CHUNKS[2:10]:
        pieces[p, d, h] = copy(piece(p, d, h), landing(p, d, h), along(p, d))
    for h in range(2):
        for i in range(2):
            for p in range(2):
                side, columns = pl.ds(2 * i, 2), pl.ds(h * BLK, BLK)
                if p == 0:
                    src = tail.at[side, (y + 2) % 4, pl.ds(0, LEN[0]), columns]
                else:
                    src = tail.at[(z + 2) % 4, side, pl.ds(LEN[0], LEN[1]), columns]
                dst = fwd.at[p, h, i, :, pl.ds(0, LEN[p]), :]
                hops[p, h, i] = copy(src, dst, along(p, 1 + 2 * i))

    def relay(p, h):
        for i in range(2):
            hops[p, h, i].wait_recv()
            src = fwd.at[p, h, i, :, pl.ds(0, LEN[p]), :]
            dst = tbuf.at[p, 2, h, pl.ds(2 * i, 2), pl.ds(0, LEN[p]), :]
            far[p, h, i] = copy(src, dst, along(p, 1 + 2 * i))

    for made in over_z:
        made.wait_recv()

    rows = lax.broadcasted_iota(jnp.int32, (BLK, BLK), 0)
    cols = lax.broadcasted_iota(jnp.int32, (BLK, BLK), 1)
    eye = jnp.where(rows == cols, 1.0, 0.0).astype(F32)
    own_cols = aligned(row * BLK, BLK, BLK)
    diagonal = wrow[:, own_cols]
    on_diag = jnp.where(rows == cols, diagonal, 0.0)
    diag_rows = jnp.sum(on_diag, axis=1, keepdims=True)
    diag_cols = jnp.sum(on_diag, axis=0, keepdims=True)
    lower = jnp.where(rows > cols, diagonal, 0.0) / diag_rows
    inverse, power = eye - lower, dot(lower, lower, HIGHEST)
    for _ in range(6):
        both = dot(jnp.concatenate([inverse, power], axis=0), power, HIGHEST)
        inverse, power = inverse + both[:BLK], both[BLK:]
    inverse = inverse / diag_cols
    gfull[row] = dot(inverse, wrow[...], HIGHEST)
    gfull[row, :, own_cols] = inverse
    over_x = [copy(gfull.at[row], gfull.at[row], where(dx=i)) for i in (1, 3, 2)]
    to_other = [copy(gfull.at[row], gfull.at[row], where(dc=1))]

    def split_panel(p, slot):
        @pl.loop(0, 2)
        def _(step):
            high, low = split(lbuf[p, slot, aligned(step * BLK, BLK, BLK), :])
            lsplit[p, aligned(slot * PART + step * BLK, BLK, BLK), :] = low
            lsplit[p, aligned(DEEP + slot * PART + step * BLK, BLK, BLK), :] = high

    def turn(p, i, d, h, slots):
        @pl.loop(*slots)
        def _(step):
            high, low = split(tbuf[p, d, h, step].T)
            tt[p, pl.ds(i * BLK, BLK), aligned(step * PART, PART, PART)] = high
            tt[p, pl.ds(i * BLK, BLK), aligned(DEEP + step * PART, PART, PART)] = low

    def add_own(p, slot):
        high_at, low_at = aligned(slot * PART, PART, PART), aligned(DEEP + slot * PART, PART, PART)

        @pl.loop(0, 4)
        def _(step):
            at = aligned(step * 256, 256, 256)
            value = dot(tt[p, :, low_at], lsplit[p, low_at, at]) + dot(tt[p, :, high_at], lsplit[p, high_at, at])
            value += dot(tt[p, :, high_at], lsplit[p, low_at, at])
            cbuf[0, :, at] += value[:BLK]
            cbuf[1, :, at] += value[BLK:]

    for made in own_panel + own_tail:
        made.wait()
    own_rhs.wait()
    turned = rhs_in[...].T
    for h in range(2):
        cbuf[h] = jnp.zeros((BLK, WIN), F32)
        cbuf[h, :, own_cols] = -turned[h * BLK : (h + 1) * BLK]
    for p in range(2):
        split_panel(p, place[p])
        for h in range(2):
            turn(p, h, 0, h, (0, 4))
    for p in (1, 0):
        for made in second[1 - p]:
            made.wait_recv()
        split_panel(p, (place[p] + 3) % 4)
        split_panel(p, (place[p] + 1) % 4)

        @pl.loop(0, 3)
        def _(i):
            add_own(p, (place[p] + 3 + i) % 4)

    for p in (1, 0):
        for made in onward[2 * (1 - p) : 2 * (1 - p) + 2]:
            made.wait_recv()
        split_panel(p, (place[p] + 2) % 4)
        add_own(p, (place[p] + 2) % 4)

    keep, give = aligned(core * 64, 64, 64), aligned((1 - core) * 64, 64, 64)
    pair, ringed, third = {}, {}, {}

    def to_pair(q):
        pair[q] = copy(cbuf.at[q, give, :], r1.at[q], where(dc=1))

    def to_ring(q):
        pair[q].wait_recv()
        part[q] = (cbuf[q, keep, :] + r1[q]).reshape(4, QUARTER, WIN)
        ringed[q] = [copy(part.at[q, (x + i) % 4], ring.at[q, i - 1], where(dx=i)) for i in (2, 1, 3)]

    def from_ring(q):
        for made in ringed[q]:
            made.wait_recv()
        psum[q] = part[q, x] + ring[q, 0] + ring[q, 1] + ring[q, 2]

    def to_owner(q):
        p, d, _ = CHUNKS[q]
        third[q] = copy(psum.at[q], r3.at[q - 2], along(p, -d))

    def near_product(p, h):
        for i, d in enumerate((1, 3)):
            turn(p, i, d, h, (0, 4))
        numbers = NUMBER[p, 1, h], NUMBER[p, 3, h]

        @pl.loop(0, 4)
        def _(step):
            at = aligned(step * 256, 256, 256)
            value = dot(tt[p], lsplit[p, :, at]) + dot(tt[p, :, :DEEP], lsplit[p, DEEP:, at])
            for i, q in enumerate(numbers):
                cbuf[q, :, at] = value[i * BLK : (i + 1) * BLK]

        for q in numbers:
            to_pair(q)

    def far_product(p, h):
        for i in range(2):
            far[p, h, i].wait_recv()
        turn(p, 0, 2, h, (0, 4))
        q = NUMBER[p, 2, h]

        @pl.loop(0, 4)
        def _(step):
            at = aligned(step * 256, 256, 256)
            value = dot(tt[p, :BLK, :], lsplit[p, :, at]) + dot(tt[p, :BLK, :DEEP], lsplit[p, DEEP:, at])
            cbuf[q, :, at] = value

        to_pair(q)

    def near_arrived(p, h):
        for d in (1, 3):
            pieces[p, d, h].wait_recv()

    to_pair(0)
    to_pair(1)
    near_arrived(0, 0)
    near_product(0, 0)
    to_ring(0)
    to_ring(1)
    for made, i in zip(over_x, (1, 3, 2)):
        made.wait_recv()
        slot = 2 * ((x - i + 4) % 4) + core
        to_other.append(copy(gfull.at[slot], gfull.at[slot], where(dc=1)))
    near_arrived(1, 0)
    near_product(1, 0)
    for q in (2, 4, 3, 5):
        to_ring(q)
    near_arrived(0, 1)
    near_product(0, 1)
    near_arrived(1, 1)
    near_product(1, 1)
    relay(0, 0)
    relay(1, 0)
    for q in (6, 8, 7, 9):
        to_ring(q)
    from_ring(0)
    from_ring(1)
    for made in to_other:
        made.wait_recv()

    @pl.loop(0, 8)
    def _(step):
        high, low = split(gfull[step])
        gsplit[0, step] = high
        gsplit[1, step] = low

    relay(0, 1)
    relay(1, 1)
    for q in (2, 4, 3, 5):
        from_ring(q)
    for p in range(2):
        far_product(p, 0)
    for q in (6, 8, 7, 9):
        from_ring(q)
    to_ring(10)
    to_ring(11)
    far_product(0, 1)
    for q in (2, 4, 6, 8):
        to_owner(q)
    to_ring(12)
    far_product(1, 1)
    for q in (3, 5, 7, 9):
        to_owner(q)
    to_ring(13)
    for q in (10, 11, 12, 13):
        from_ring(q)
        to_owner(q)
    totals = []
    for h in range(2):
        total = psum[h]
        for d in (1, 3, 2):
            for p in range(2):
                q = NUMBER[p, d, h]
                third[q].wait_recv()
                total += r3[q - 2]
        totals.append(total)

    left = -jnp.concatenate(totals, axis=0)
    for j in range(7, -1, -1):
        high, low = split(left[:, j * BLK : (j + 1) * BLK])
        width = (j + 1) * BLK
        both = dot(jnp.concatenate([high, low], axis=0), gsplit[0, j, :, :width])
        step = both[:32] + both[32:] + dot(high, gsplit[1, j, :, :width])
        xs[j] = step[:, j * BLK :].reshape(2, QUARTER, BLK)
        if j:
            left = left[:, : j * BLK] - step[:, : j * BLK]

    own = aligned(core * 64 + x * QUARTER, QUARTER, QUARTER)
    obuf[:, own, :] = xs[row]
    spread = []
    for i in range(4):
        for j in range(2):
            if (i, j) != (0, 0):
                target = where(dx=i, dc=j)
                spread.append(copy(xs.at[target[0]], obuf.at[:, own, :], target))
    for made in spread:
        made.wait_recv()
    out[...] = obuf[...].reshape(COLS, BLK).T
    for made in started:
        made.wait_send()


def per_device(tail_vectors, lower_panel, window_rhs, window_block):
    anywhere = pl.BlockSpec(memory_space=pl.ANY)
    count = len(CHUNKS)
    return pl.pallas_call(
        kernel,
        name="window_solve",
        out_shape=jax.ShapeDtypeStruct((BLK, COLS), F32),
        in_specs=[anywhere] * 4,
        out_specs=pl.BlockSpec(memory_space=pltpu.VMEM),
        scratch_shapes=[
            pltpu.VMEM((2, 4, 2, 4, PART, BLK), F32),
            pltpu.VMEM((2, 2, 2, 2, PART, BLK), F32),
            pltpu.VMEM((2, 4, PART, WIN), F32),
            pltpu.VMEM((2, 2 * DEEP, WIN), BF16),
            pltpu.VMEM((2, COLS, 2 * DEEP), BF16),
            pltpu.VMEM((count, BLK, WIN), F32),
            pltpu.VMEM((BLK, WIN), F32),
            pltpu.VMEM((8, BLK, WIN), F32),
            pltpu.VMEM((2, 8, BLK, WIN), BF16),
            pltpu.VMEM((BLK, COLS), F32),
            pltpu.VMEM((count, 64, WIN), F32),
            pltpu.VMEM((count, 4, QUARTER, WIN), F32),
            pltpu.VMEM((count, 3, QUARTER, WIN), F32),
            pltpu.VMEM((count, QUARTER, WIN), F32),
            pltpu.VMEM((count - 2, QUARTER, WIN), F32),
            pltpu.VMEM((8, 2, QUARTER, BLK), F32),
            pltpu.VMEM((2, BLK, BLK), F32),
            pltpu.SemaphoreType.DMA((COPIES,)),
            pltpu.SemaphoreType.DMA((COPIES,)),
            pltpu.SemaphoreType.DMA((8,)),
        ],
        compiler_params=pltpu.CompilerParams(
            collective_id=0, has_side_effects=True, vmem_limit_bytes=62 * 1024 * 1024
        ),
    )(tail_vectors.reshape(4, 4, SEG, COLS), lower_panel, window_rhs, window_block)


def solution(mesh):
    in_specs = (P("row", "col"), P(("row", "col"), None), P("row", "col"), P(("row", "col"), None))
    return jax.shard_map(
        per_device, mesh=mesh, in_specs=in_specs, out_specs=P("row", "col"), check_vma=False
    )
```

```python
import jax
import jax.numpy as jnp
from jax import lax
from jax.experimental import pallas as pl
from jax.experimental.pallas import tpu as pltpu
from jax.sharding import PartitionSpec as P

F32, BF16 = jnp.float32, jnp.bfloat16
HIGHEST = lax.Precision.HIGHEST
SEG = 504
LEN = (256, 248)
PART = 256
DEEP = 4 * PART
WIN = 1024
COLS = 256
BLK = 128
QUARTER = 16
CHUNKS = [(None, 0, 0), (None, 0, 1)] + [(p, d, h) for near in ((1, 3), (2,)) for h in range(2) for d in near for p in range(2)]
NUMBER = {chunk: q for q, chunk in enumerate(CHUNKS)}
SLOT = (0, 1, 3, 2)
RECEIVED, SENDING, LOCAL = 62, 15, 8


def split(value):
    high = value.astype(BF16)
    return high, (value - high.astype(F32)).astype(BF16)


def dot(a, b, precision=None):
    return jnp.dot(a, b, preferred_element_type=F32, precision=precision)


def aligned(start, size, unit):
    return pl.ds(pl.multiple_of(start, unit), size)


def kernel(
    tail, panel, rhs, block, out,
    tbuf, fwd, lbuf, lsplit, tt, cbuf, wrow, gfull, gsplit, rhs_in,
    r1, part, ring, psum, r3, xs, obuf,
    send_sem, recv_sem, local_sem,
):
    row, col = lax.axis_index("row"), lax.axis_index("col")
    x, core = row // 2, row % 2
    z, y = col // 4, col % 4

    def where(dx=0, dc=0, dz=0, dy=0):
        new_row = 2 * ((x + dx + 4) % 4) + (core + dc) % 2
        new_col = 4 * ((z + dz + 4) % 4) + (y + dy + 4) % 4
        return (new_row, new_col)

    def along(p, step):
        return where(dy=step) if p == 0 else where(dz=step)

    def across(p, step):
        return along(1 - p, step)

    place = (z, y)

    received, sending = {}, {}

    def copy(src, dst, target, group, sent):
        at, out_at = received.setdefault(group, len(received)), sending.setdefault(sent, len(sending))
        pltpu.make_async_remote_copy(
            src_ref=src,
            dst_ref=dst,
            send_sem=send_sem.at[out_at],
            recv_sem=recv_sem.at[at],
            device_id=target,
            device_id_type=pl.DeviceIdType.MESH,
        ).start()

    def arrived(group, ref):
        pltpu.make_async_copy(ref, ref, recv_sem.at[received[group]]).wait()

    def gone(sent, ref):
        pltpu.make_async_copy(ref, ref, send_sem.at[sending[sent]]).wait()

    local = []

    def bring(src, dst):
        made = pltpu.make_async_copy(src, dst, local_sem.at[len(local)])
        made.start()
        local.append(made)
        return made

    def piece(p, step, h):
        columns = pl.ds(h * BLK, BLK)
        if p == 0:
            return tail.at[:, (y + step) % 4, pl.ds(0, LEN[0]), columns]
        return tail.at[(z + step) % 4, :, pl.ds(LEN[0], LEN[1]), columns]

    def landing(p, d, h):
        return tbuf.at[p, SLOT[d], h, :, pl.ds(0, LEN[p]), :]

    partners = [where(dy=i) for i in (1, 2, 3)] + [where(dz=i) for i in (1, 2, 3)]
    partners += [where(dx=i, dc=j) for i in range(4) for j in range(2) if (i, j) != (0, 0)]
    barrier = pltpu.get_barrier_semaphore()
    for partner in partners:
        pl.semaphore_signal(barrier, inc=1, device_id=partner, device_id_type=pl.DeviceIdType.MESH)
    pl.semaphore_wait(barrier, len(partners))

    lanes = pl.ds(0, WIN // 2), pl.ds(WIN // 2, WIN // 2)
    for i in (1, 3, 2):
        for p in range(2):
            copy(block.at[:, lanes[p]], wrow.at[z, y, :, lanes[p]], along(p, i), "shards", "shards")

    def half(p, side):
        return pl.ds(0, 128) if side == 0 else pl.ds(128, LEN[p] - 128)

    def send_panel(p, step, side, group):
        src = pl.ds(p * PART + half(p, side).start, half(p, side).size)
        copy(panel.at[src, :], lbuf.at[p, place[p], half(p, side), :], across(p, step), group, ("panel", p))

    for p in (1, 0):
        send_panel(p, 1, 0, ("up", p))
        send_panel(p, 3, 1, ("down", p))
    own_block = bring(block, wrow.at[z, y])
    own_panel = [
        bring(panel.at[pl.ds(p * PART, LEN[p]), :], lbuf.at[p, place[p], pl.ds(0, LEN[p]), :]) for p in range(2)
    ]
    own_rhs = bring(rhs, rhs_in)
    own_tail = [bring(piece(p, 0, h), landing(p, 0, h)) for p in range(2) for h in range(2)]

    for i in range(4):
        lbuf[1, i, LEN[1] :, :] = jnp.zeros((PART - LEN[1], WIN), F32)
        for d in range(4):
            for h in range(2):
                tbuf[1, d, h, i, LEN[1] :, :] = jnp.zeros((PART - LEN[1], BLK), F32)

    own_block.wait()
    arrived("shards", wrow.at[0, pl.ds(0, 3)])
    for i in (1, 3, 2):
        at = wrow.at[z, :, :, lanes[0]]
        copy(at, at, where(dz=i), "rows", "rows")
        at = wrow.at[:, y, :, lanes[1]]
        copy(at, at, where(dy=i), "rows", "rows")
    for p in (1, 0):
        send_panel(p, 1, 1, ("second", p))
        send_panel(p, 3, 0, ("second", p))

    for p in (1, 0):
        for name, step, side in (("up", 1, 0), ("down", 3, 1)):
            at = lbuf.at[p, (place[p] - step + 4) % 4, half(p, side), :]
            arrived((name, p), at)
            copy(at, at, across(p, step), ("onward", p), ("panel", p))

    for p, d, h in CHUNKS[2:10]:
        copy(piece(p, d, h), landing(p, d, h), along(p, d), ("near", p, h), ("near", p))
    for h in range(2):
        for i in range(2):
            for p in range(2):
                side, columns = pl.ds(2 * i, 2), pl.ds(h * BLK, BLK)
                if p == 0:
                    src = tail.at[side, (y + 2) % 4, pl.ds(0, LEN[0]), columns]
                else:
                    src = tail.at[(z + 2) % 4, side, pl.ds(LEN[0], LEN[1]), columns]
                dst = fwd.at[p, h, i, :, pl.ds(0, LEN[p]), :]
                copy(src, dst, along(p, 1 + 2 * i), ("hop", p, h), ("hop", p))

    def relay(p, h):
        arrived(("hop", p, h), fwd.at[p, h, :, :, pl.ds(0, LEN[p]), :])
        for i in range(2):
            src = fwd.at[p, h, i, :, pl.ds(0, LEN[p]), :]
            dst = tbuf.at[p, SLOT[2], h, pl.ds(2 * i, 2), pl.ds(0, LEN[p]), :]
            copy(src, dst, along(p, 1 + 2 * i), ("far", p, h), ("far", p))

    arrived("rows", wrow.at[pl.ds(0, 3)])

    rows = lax.broadcasted_iota(jnp.int32, (BLK, BLK), 0)
    cols = lax.broadcasted_iota(jnp.int32, (BLK, BLK), 1)
    eye = jnp.where(rows == cols, 1.0, 0.0).astype(F32)
    own_cols = aligned(row * BLK, BLK, BLK)
    diagonal = wrow[:, :, :, own_cols].reshape(BLK, BLK)
    on_diag = jnp.where(rows == cols, diagonal, 0.0)
    diag_rows = jnp.sum(on_diag, axis=1, keepdims=True)
    diag_cols = jnp.sum(on_diag, axis=0, keepdims=True)
    lower = jnp.where(rows > cols, diagonal, 0.0) / diag_rows
    inverse, power = eye - lower, dot(lower, lower, HIGHEST)
    for _ in range(6):
        both = dot(jnp.concatenate([inverse, power], axis=0), power, HIGHEST)
        inverse, power = inverse + both[:BLK], both[BLK:]
    inverse = inverse / diag_cols
    gfull[row] = dot(inverse, wrow[...].reshape(BLK, WIN), HIGHEST)
    gfull[row, :, own_cols] = inverse
    for i in (1, 3, 2):
        copy(gfull.at[row], gfull.at[row], where(dx=i), "over_x", "blocks")
    copy(gfull.at[row], gfull.at[row], where(dc=1), "to_other", "blocks")

    def split_panel(p, slot):
        @pl.loop(0, 2)
        def _(step):
            high, low = split(lbuf[p, slot, aligned(step * BLK, BLK, BLK), :])
            lsplit[p, aligned(slot * PART + step * BLK, BLK, BLK), :] = low
            lsplit[p, aligned(DEEP + slot * PART + step * BLK, BLK, BLK), :] = high

    def turn(p, i, d, h, slots):
        @pl.loop(*slots)
        def _(step):
            high, low = split(tbuf[p, SLOT[d], h, step].T)
            tt[p, pl.ds(i * BLK, BLK), aligned(step * PART, PART, PART)] = high
            tt[p, pl.ds(i * BLK, BLK), aligned(DEEP + step * PART, PART, PART)] = low

    def add_own(p, slot):
        high_at, low_at = aligned(slot * PART, PART, PART), aligned(DEEP + slot * PART, PART, PART)

        @pl.loop(0, 4)
        def _(step):
            at = aligned(step * 256, 256, 256)
            value = dot(tt[p, :, low_at], lsplit[p, low_at, at]) + dot(tt[p, :, high_at], lsplit[p, high_at, at])
            value += dot(tt[p, :, high_at], lsplit[p, low_at, at])
            cbuf[0, :, at] += value[:BLK]
            cbuf[1, :, at] += value[BLK:]

    for made in own_panel + own_tail:
        made.wait()
    own_rhs.wait()
    turned = rhs_in[...].T
    for h in range(2):
        cbuf[h] = jnp.zeros((BLK, WIN), F32)
        cbuf[h, :, own_cols] = -turned[h * BLK : (h + 1) * BLK]
    for p in range(2):
        split_panel(p, place[p])
        for h in range(2):
            turn(p, h, 0, h, (0, 4))
    for p in (1, 0):
        arrived(("second", p), lbuf.at[p, 0, pl.ds(0, LEN[p]), :])
        split_panel(p, (place[p] + 3) % 4)
        split_panel(p, (place[p] + 1) % 4)

        @pl.loop(0, 3)
        def _(i):
            add_own(p, (place[p] + 3 + i) % 4)

    for p in (1, 0):
        arrived(("onward", p), lbuf.at[p, 0, pl.ds(0, LEN[p]), :])
        split_panel(p, (place[p] + 2) % 4)
        add_own(p, (place[p] + 2) % 4)

    keep, give = aligned(core * 64, 64, 64), aligned((1 - core) * 64, 64, 64)

    def to_pair(q):
        copy(cbuf.at[q, give, :], r1.at[q], where(dc=1), ("pair", q), "pair")

    def to_ring(q):
        arrived(("pair", q), r1.at[q])
        part[q] = (cbuf[q, keep, :] + r1[q]).reshape(4, QUARTER, WIN)
        for i in (2, 1, 3):
            copy(part.at[q, (x + i) % 4], ring.at[q, i - 1], where(dx=i), ("ring", q), "ring")

    def from_ring(q):
        arrived(("ring", q), ring.at[q])
        psum[q] = part[q, x] + ring[q, 0] + ring[q, 1] + ring[q, 2]

    def to_owner(q):
        p, d, _ = CHUNKS[q]
        copy(psum.at[q], r3.at[q - 2], along(p, -d), "owner", "owner")

    def near_product(p, h):
        for i, d in enumerate((1, 3)):
            turn(p, i, d, h, (0, 4))
        numbers = NUMBER[p, 1, h], NUMBER[p, 3, h]

        @pl.loop(0, 4)
        def _(step):
            at = aligned(step * 256, 256, 256)
            value = dot(tt[p], lsplit[p, :, at]) + dot(tt[p, :, :DEEP], lsplit[p, DEEP:, at])
            for i, q in enumerate(numbers):
                cbuf[q, :, at] = value[i * BLK : (i + 1) * BLK]

        for q in numbers:
            to_pair(q)

    def far_product(p, h, s):
        if s:
            arrived(("far", p, h), landing(p, 2, h))
            turn(p, 0, 2, h, (0, 4))
        q = NUMBER[p, 2, h]

        @pl.loop(2 * s, 2 * s + 2)
        def _(step):
            at = aligned(step * 256, 256, 256)
            value = dot(tt[p, :BLK, :], lsplit[p, :, at]) + dot(tt[p, :BLK, :DEEP], lsplit[p, DEEP:, at])
            cbuf[q, :, at] = value

        copy(cbuf.at[q, give, lanes[s]], r1.at[q, :, lanes[s]], where(dc=1), ("pair", q, s), "pair")

    def to_ring_half(q, s):
        arrived(("pair", q, s), r1.at[q, :, lanes[s]])
        value = cbuf[q, keep, lanes[s]] + r1[q, :, lanes[s]]
        part[q, :, :, lanes[s]] = value.reshape(4, QUARTER, WIN // 2)
        for i in (2, 1, 3):
            src, dst = part.at[q, (x + i) % 4, :, lanes[s]], ring.at[q, i - 1, :, lanes[s]]
            copy(src, dst, where(dx=i), ("ring", q, s), "ring")

    def from_ring_half(q, s):
        at = lanes[s]
        arrived(("ring", q, s), ring.at[q, :, :, at])
        psum[q, :, at] = part[q, x, :, at] + ring[q, 0, :, at] + ring[q, 1, :, at] + ring[q, 2, :, at]
        p, d, _ = CHUNKS[q]
        copy(psum.at[q, :, at], r3.at[q - 2, :, at], along(p, -d), "owner", "owner")

    def near_arrived(p, h):
        arrived(("near", p, h), tbuf.at[p, pl.ds(1, 2), h, :, pl.ds(0, LEN[p]), :])

    to_pair(0)
    to_pair(1)
    to_ring(0)
    to_ring(1)
    near_arrived(0, 0)
    near_product(0, 0)
    arrived("over_x", gfull.at[pl.ds(0, 3)])
    for i in (1, 3, 2):
        slot = 2 * ((x - i + 4) % 4) + core
        copy(gfull.at[slot], gfull.at[slot], where(dc=1), "to_other", "blocks")
    near_arrived(1, 0)
    near_product(1, 0)
    for q in (2, 4, 3, 5):
        to_ring(q)
    near_arrived(0, 1)
    near_product(0, 1)
    near_arrived(1, 1)
    near_product(1, 1)
    relay(0, 0)
    relay(1, 0)
    for q in (6, 8, 7, 9):
        to_ring(q)
    from_ring(0)
    from_ring(1)
    arrived("to_other", gfull.at[pl.ds(0, 4)])

    @pl.loop(0, 8)
    def _(step):
        high, low = split(gfull[step])
        gsplit[0, step] = high
        gsplit[1, step] = low

    relay(0, 1)
    relay(1, 1)
    for q in (2, 4, 3, 5):
        from_ring(q)
    far_product(0, 0, 1)
    far_product(0, 0, 0)
    far_product(1, 0, 1)
    to_ring_half(10, 1)
    far_product(1, 0, 0)
    to_ring_half(10, 0)
    to_ring_half(11, 1)
    to_ring_half(11, 0)
    for q in (6, 8, 7, 9):
        from_ring(q)
    far_product(0, 1, 1)
    far_product(0, 1, 0)
    for q in (2, 4, 6, 8):
        to_owner(q)
    to_ring_half(12, 1)
    far_product(1, 1, 1)
    to_ring_half(12, 0)
    far_product(1, 1, 0)
    for q in (3, 5, 7, 9):
        to_owner(q)
    to_ring_half(13, 1)
    to_ring_half(13, 0)
    for q in (10, 11, 12, 13):
        for s in (1, 0):
            from_ring_half(q, s)
    arrived("owner", r3)
    totals = []
    for h in range(2):
        total = psum[h]
        for d in (1, 3, 2):
            for p in range(2):
                q = NUMBER[p, d, h]
                total += r3[q - 2]
        totals.append(total)

    left = -jnp.concatenate(totals, axis=0)
    for j in range(7, -1, -1):
        high, low = split(left[:, j * BLK : (j + 1) * BLK])
        width = (j + 1) * BLK
        both = dot(jnp.concatenate([high, low], axis=0), gsplit[0, j, :, :width])
        step = both[:32] + both[32:] + dot(high, gsplit[1, j, :, :width])
        xs[j] = step[:, j * BLK :].reshape(2, QUARTER, BLK)
        if j:
            left = left[:, : j * BLK] - step[:, : j * BLK]

    own = aligned(core * 64 + x * QUARTER, QUARTER, QUARTER)
    obuf[:, own, :] = xs[row]
    for i in range(4):
        for j in range(2):
            if (i, j) != (0, 0):
                target = where(dx=i, dc=j)
                copy(xs.at[target[0]], obuf.at[:, own, :], target, "spread", "spread")
    arrived("spread", xs.at[pl.ds(0, 7)])
    out[...] = obuf[...].reshape(COLS, BLK).T
    gone("shards", wrow.at[0, pl.ds(0, 3)])
    gone("rows", wrow.at[pl.ds(0, 3)])
    gone("blocks", gfull.at[pl.ds(0, 7)])
    for p in range(2):
        gone(("panel", p), lbuf.at[p, pl.ds(0, 3), pl.ds(0, LEN[p]), :])
        gone(("near", p), tbuf.at[p, pl.ds(1, 2), :, :, pl.ds(0, LEN[p]), :])
        gone(("hop", p), fwd.at[p, :, :, :, pl.ds(0, LEN[p]), :])
        gone(("far", p), tbuf.at[p, SLOT[2], :, :, pl.ds(0, LEN[p]), :])
    gone("pair", r1)
    gone("ring", ring)
    gone("owner", r3)
    gone("spread", xs.at[pl.ds(0, 7)])
    assert len(received) == RECEIVED and len(sending) == SENDING


def per_device(tail_vectors, lower_panel, window_rhs, window_block):
    anywhere = pl.BlockSpec(memory_space=pl.ANY)
    count = len(CHUNKS)
    return pl.pallas_call(
        kernel,
        name="window_solve",
        out_shape=jax.ShapeDtypeStruct((BLK, COLS), F32),
        in_specs=[anywhere] * 4,
        out_specs=pl.BlockSpec(memory_space=pltpu.VMEM),
        scratch_shapes=[
            pltpu.VMEM((2, 4, 2, 4, PART, BLK), F32),
            pltpu.VMEM((2, 2, 2, 2, PART, BLK), F32),
            pltpu.VMEM((2, 4, PART, WIN), F32),
            pltpu.VMEM((2, 2 * DEEP, WIN), BF16),
            pltpu.VMEM((2, COLS, 2 * DEEP), BF16),
            pltpu.VMEM((count, BLK, WIN), F32),
            pltpu.VMEM((4, 4, 8, WIN), F32),
            pltpu.VMEM((8, BLK, WIN), F32),
            pltpu.VMEM((2, 8, BLK, WIN), BF16),
            pltpu.VMEM((BLK, COLS), F32),
            pltpu.VMEM((count, 64, WIN), F32),
            pltpu.VMEM((count, 4, QUARTER, WIN), F32),
            pltpu.VMEM((count, 3, QUARTER, WIN), F32),
            pltpu.VMEM((count, QUARTER, WIN), F32),
            pltpu.VMEM((count - 2, QUARTER, WIN), F32),
            pltpu.VMEM((8, 2, QUARTER, BLK), F32),
            pltpu.VMEM((2, BLK, BLK), F32),
            pltpu.SemaphoreType.DMA((SENDING,)),
            pltpu.SemaphoreType.DMA((RECEIVED,)),
            pltpu.SemaphoreType.DMA((LOCAL,)),
        ],
        compiler_params=pltpu.CompilerParams(
            collective_id=0, has_side_effects=True, vmem_limit_bytes=62 * 1024 * 1024
        ),
    )(tail_vectors.reshape(4, 4, SEG, COLS), lower_panel, window_rhs, window_block)


def solution(mesh):
    in_specs = (P("row", "col"), P(("row", "col"), None), P("row", "col"), P(("row", "col"), None))
    return jax.shard_map(
        per_device, mesh=mesh, in_specs=in_specs, out_specs=P("row", "col"), check_vma=False
    )
```

```python
import jax
import jax.numpy as jnp
from jax import lax
from jax.experimental import pallas as pl
from jax.experimental.pallas import tpu as pltpu
from jax.sharding import PartitionSpec as P

F32, BF16 = jnp.float32, jnp.bfloat16
HIGHEST = lax.Precision.HIGHEST
SEG = 504
LEN = (256, 248)
PART = 256
DEEP = 4 * PART
WIN = 1024
COLS = 256
BLK = 128
QUARTER = 16
CHUNKS = [(None, 0, 0), (None, 0, 1)] + [(p, d, h) for near in ((1, 3), (2,)) for h in range(2) for p in range(2) for d in near]
NUMBER = {chunk: q for q, chunk in enumerate(CHUNKS)}
SLOT = (0, 1, 3, 2)
RECEIVED, SENDING, LOCAL = 62, 15, 8


def split(value):
    high = value.astype(BF16)
    return high, (value - high.astype(F32)).astype(BF16)


def dot(a, b, precision=None):
    return jnp.dot(a, b, preferred_element_type=F32, precision=precision)


def aligned(start, size, unit):
    return pl.ds(pl.multiple_of(start, unit), size)


def kernel(
    tail, panel, rhs, block, out,
    tbuf, fwd, lbuf, lsplit, tt, cbuf, wrow, gfull, gsplit, rhs_in,
    r1, part, ring, psum, r3, xs, obuf,
    send_sem, recv_sem, local_sem,
):
    row, col = lax.axis_index("row"), lax.axis_index("col")
    x, core = row // 2, row % 2
    z, y = col // 4, col % 4

    def where(dx=0, dc=0, dz=0, dy=0):
        new_row = 2 * ((x + dx + 4) % 4) + (core + dc) % 2
        new_col = 4 * ((z + dz + 4) % 4) + (y + dy + 4) % 4
        return (new_row, new_col)

    def along(p, step):
        return where(dy=step) if p == 0 else where(dz=step)

    def across(p, step):
        return along(1 - p, step)

    place = (z, y)

    received, sending = {}, {}

    def copy(src, dst, target, group, sent):
        at, out_at = received.setdefault(group, len(received)), sending.setdefault(sent, len(sending))
        pltpu.make_async_remote_copy(
            src_ref=src,
            dst_ref=dst,
            send_sem=send_sem.at[out_at],
            recv_sem=recv_sem.at[at],
            device_id=target,
            device_id_type=pl.DeviceIdType.MESH,
        ).start()

    def arrived(group, ref):
        pltpu.make_async_copy(ref, ref, recv_sem.at[received[group]]).wait()

    def gone(sent, ref):
        pltpu.make_async_copy(ref, ref, send_sem.at[sending[sent]]).wait()

    local = []

    def bring(src, dst):
        made = pltpu.make_async_copy(src, dst, local_sem.at[len(local)])
        made.start()
        local.append(made)
        return made

    def piece(p, step, h):
        columns = pl.ds(h * BLK, BLK)
        if p == 0:
            return tail.at[:, (y + step) % 4, pl.ds(0, LEN[0]), columns]
        return tail.at[(z + step) % 4, :, pl.ds(LEN[0], LEN[1]), columns]

    def landing(p, d, h):
        return tbuf.at[p, SLOT[d], h, :, pl.ds(0, LEN[p]), :]

    partners = [where(dy=i) for i in (1, 2, 3)] + [where(dz=i) for i in (1, 2, 3)]
    partners += [where(dx=i, dc=j) for i in range(4) for j in range(2) if (i, j) != (0, 0)]
    barrier = pltpu.get_barrier_semaphore()
    for partner in partners:
        pl.semaphore_signal(barrier, inc=1, device_id=partner, device_id_type=pl.DeviceIdType.MESH)
    pl.semaphore_wait(barrier, len(partners))

    lanes = pl.ds(0, WIN // 2), pl.ds(WIN // 2, WIN // 2)
    for i in (1, 3, 2):
        copy(block, wrow.at[z, y], where(dy=i), "shards", "shards")

    def half(p, side):
        return pl.ds(0, 128) if side == 0 else pl.ds(128, LEN[p] - 128)

    def send_panel(p, step, side, group):
        src = pl.ds(p * PART + half(p, side).start, half(p, side).size)
        copy(panel.at[src, :], lbuf.at[p, place[p], half(p, side), :], across(p, step), group, ("panel", p))

    for p in (1, 0):
        send_panel(p, 1, 0, ("up", p))
        send_panel(p, 3, 1, ("down", p))
    own_block = bring(block, wrow.at[z, y])
    own_panel = [
        bring(panel.at[pl.ds(p * PART, LEN[p]), :], lbuf.at[p, place[p], pl.ds(0, LEN[p]), :]) for p in range(2)
    ]
    own_rhs = bring(rhs, rhs_in)
    own_tail = [bring(piece(p, 0, h), landing(p, 0, h)) for p in range(2) for h in range(2)]

    for i in range(4):
        lbuf[1, i, LEN[1] :, :] = jnp.zeros((PART - LEN[1], WIN), F32)
        for d in range(4):
            for h in range(2):
                tbuf[1, d, h, i, LEN[1] :, :] = jnp.zeros((PART - LEN[1], BLK), F32)

    own_block.wait()
    arrived("shards", wrow.at[0, pl.ds(0, 3)])
    for i in (1, 3, 2):
        copy(wrow.at[z], wrow.at[z], where(dz=i), "rows", "rows")
    for p in (1, 0):
        send_panel(p, 1, 1, ("second", p))
        send_panel(p, 3, 0, ("second", p))

    for p in (1, 0):
        for name, step, side in (("up", 1, 0), ("down", 3, 1)):
            at = lbuf.at[p, (place[p] - step + 4) % 4, half(p, side), :]
            arrived((name, p), at)
            copy(at, at, across(p, step), ("onward", p), ("panel", p))

    for p, d, h in CHUNKS[2:10]:
        copy(piece(p, d, h), landing(p, d, h), along(p, d), ("near", p, h), ("near", p))
    for h in range(2):
        for i in range(2):
            for p in range(2):
                side, columns = pl.ds(2 * i, 2), pl.ds(h * BLK, BLK)
                if p == 0:
                    src = tail.at[side, (y + 2) % 4, pl.ds(0, LEN[0]), columns]
                else:
                    src = tail.at[(z + 2) % 4, side, pl.ds(LEN[0], LEN[1]), columns]
                dst = fwd.at[p, h, i, :, pl.ds(0, LEN[p]), :]
                copy(src, dst, along(p, 1 + 2 * i), ("hop", p, h), ("hop", p))

    def relay(p, h):
        arrived(("hop", p, h), fwd.at[p, h, :, :, pl.ds(0, LEN[p]), :])
        for i in range(2):
            src = fwd.at[p, h, i, :, pl.ds(0, LEN[p]), :]
            dst = tbuf.at[p, SLOT[2], h, pl.ds(2 * i, 2), pl.ds(0, LEN[p]), :]
            copy(src, dst, along(p, 1 + 2 * i), ("far", p, h), ("far", p))

    arrived("rows", wrow.at[pl.ds(0, 3)])

    rows = lax.broadcasted_iota(jnp.int32, (BLK, BLK), 0)
    cols = lax.broadcasted_iota(jnp.int32, (BLK, BLK), 1)
    eye = jnp.where(rows == cols, 1.0, 0.0).astype(F32)
    own_cols = aligned(row * BLK, BLK, BLK)
    diagonal = wrow[:, :, :, own_cols].reshape(BLK, BLK)
    on_diag = jnp.where(rows == cols, diagonal, 0.0)
    diag_rows = jnp.sum(on_diag, axis=1, keepdims=True)
    diag_cols = jnp.sum(on_diag, axis=0, keepdims=True)
    lower = jnp.where(rows > cols, diagonal, 0.0) / diag_rows
    inverse, power = eye - lower, dot(lower, lower, HIGHEST)
    for _ in range(6):
        both = dot(jnp.concatenate([inverse, power], axis=0), power, HIGHEST)
        inverse, power = inverse + both[:BLK], both[BLK:]
    inverse = inverse / diag_cols
    gfull[row] = dot(inverse, wrow[...].reshape(BLK, WIN), HIGHEST)
    gfull[row, :, own_cols] = inverse
    for i in (1, 3, 2):
        copy(gfull.at[row], gfull.at[row], where(dx=i), "over_x", "blocks")
    copy(gfull.at[row], gfull.at[row], where(dc=1), "to_other", "blocks")

    def split_panel(p, slot):
        @pl.loop(0, 2)
        def _(step):
            high, low = split(lbuf[p, slot, aligned(step * BLK, BLK, BLK), :])
            lsplit[p, aligned(slot * PART + step * BLK, BLK, BLK), :] = low
            lsplit[p, aligned(DEEP + slot * PART + step * BLK, BLK, BLK), :] = high

    def turn(p, i, d, h, slots):
        @pl.loop(*slots)
        def _(step):
            high, low = split(tbuf[p, SLOT[d], h, step].T)
            tt[p, pl.ds(i * BLK, BLK), aligned(step * PART, PART, PART)] = high
            tt[p, pl.ds(i * BLK, BLK), aligned(DEEP + step * PART, PART, PART)] = low

    def add_own(p, slot):
        high_at, low_at = aligned(slot * PART, PART, PART), aligned(DEEP + slot * PART, PART, PART)

        @pl.loop(0, 4)
        def _(step):
            at = aligned(step * 256, 256, 256)
            value = dot(tt[p, :, low_at], lsplit[p, low_at, at]) + dot(tt[p, :, high_at], lsplit[p, high_at, at])
            value += dot(tt[p, :, high_at], lsplit[p, low_at, at])
            cbuf[0, :, at] += value[:BLK]
            cbuf[1, :, at] += value[BLK:]

    for made in own_panel + own_tail:
        made.wait()
    own_rhs.wait()
    turned = rhs_in[...].T
    for h in range(2):
        cbuf[h] = jnp.zeros((BLK, WIN), F32)
        cbuf[h, :, own_cols] = -turned[h * BLK : (h + 1) * BLK]
    for p in range(2):
        split_panel(p, place[p])
        for h in range(2):
            turn(p, h, 0, h, (0, 4))
    for p in (1, 0):
        arrived(("second", p), lbuf.at[p, 0, pl.ds(0, LEN[p]), :])
        split_panel(p, (place[p] + 3) % 4)
        split_panel(p, (place[p] + 1) % 4)

        @pl.loop(0, 3)
        def _(i):
            add_own(p, (place[p] + 3 + i) % 4)

    for p in (1, 0):
        arrived(("onward", p), lbuf.at[p, 0, pl.ds(0, LEN[p]), :])
        split_panel(p, (place[p] + 2) % 4)
        add_own(p, (place[p] + 2) % 4)

    keep, give = aligned(core * 64, 64, 64), aligned((1 - core) * 64, 64, 64)

    def to_pair(q, n, s):
        at = pl.ds(q, n)
        copy(cbuf.at[at, give, lanes[s]], r1.at[at, :, lanes[s]], where(dc=1), ("pair", q, s), "pair")

    def to_ring(q, n, s):
        at = pl.ds(q, n)
        arrived(("pair", q, s), r1.at[at, :, lanes[s]])
        value = cbuf[at, keep, lanes[s]] + r1[at, :, lanes[s]]
        part[at, :, :, lanes[s]] = value.reshape(n, 4, QUARTER, WIN // 2)
        for i in (2, 1, 3):
            src, dst = part.at[at, (x + i) % 4, :, lanes[s]], ring.at[at, i - 1, :, lanes[s]]
            copy(src, dst, where(dx=i), ("ring", q, s), "ring")

    def from_ring(q, n, s):
        arrived(("ring", q, s), ring.at[pl.ds(q, n), :, :, lanes[s]])
        at = lanes[s]
        for k in range(q, q + n):
            psum[k, :, at] = part[k, x, :, at] + ring[k, 0, :, at] + ring[k, 1, :, at] + ring[k, 2, :, at]

    def to_owner(q, at=pl.ds(0, WIN)):
        p, d, _ = CHUNKS[q]
        copy(psum.at[q, :, at], r3.at[q - 2, :, at], along(p, -d), "owner", "owner")

    def near_product(p, h, s):
        if s:
            arrived(("near", p, h), tbuf.at[p, pl.ds(1, 2), h, :, pl.ds(0, LEN[p]), :])
            for i, d in enumerate((1, 3)):
                turn(p, i, d, h, (0, 4))
        q = NUMBER[p, 1, h]

        @pl.loop(2 * s, 2 * s + 2)
        def _(step):
            at = aligned(step * 256, 256, 256)
            value = dot(tt[p], lsplit[p, :, at]) + dot(tt[p, :, :DEEP], lsplit[p, DEEP:, at])
            for i in range(2):
                cbuf[q + i, :, at] = value[i * BLK : (i + 1) * BLK]

        to_pair(q, 2, s)

    def far_product(p, h, s):
        if s:
            arrived(("far", p, h), landing(p, 2, h))
            turn(p, 0, 2, h, (0, 4))
        q = NUMBER[p, 2, h]

        @pl.loop(2 * s, 2 * s + 2)
        def _(step):
            at = aligned(step * 256, 256, 256)
            value = dot(tt[p, :BLK, :], lsplit[p, :, at]) + dot(tt[p, :BLK, :DEEP], lsplit[p, DEEP:, at])
            cbuf[q, :, at] = value

        to_pair(q, 1, s)

    to_pair(0, 2, 1)
    to_pair(0, 2, 0)
    to_ring(0, 2, 1)
    to_ring(0, 2, 0)
    near_product(0, 0, 1)
    near_product(0, 0, 0)
    to_ring(2, 2, 1)
    near_product(1, 0, 1)
    to_ring(2, 2, 0)
    near_product(1, 0, 0)
    to_ring(4, 2, 1)
    arrived("over_x", gfull.at[pl.ds(0, 3)])
    for i in (1, 3, 2):
        slot = 2 * ((x - i + 4) % 4) + core
        copy(gfull.at[slot], gfull.at[slot], where(dc=1), "to_other", "blocks")
    to_ring(4, 2, 0)
    from_ring(0, 2, 1)
    from_ring(0, 2, 0)
    near_product(0, 1, 1)
    near_product(0, 1, 0)
    to_ring(6, 2, 1)
    near_product(1, 1, 1)
    to_ring(6, 2, 0)
    near_product(1, 1, 0)
    to_ring(8, 2, 1)
    relay(0, 0)
    relay(1, 0)
    to_ring(8, 2, 0)
    arrived("to_other", gfull.at[pl.ds(0, 4)])

    @pl.loop(0, 8)
    def _(step):
        high, low = split(gfull[step])
        gsplit[0, step] = high
        gsplit[1, step] = low

    relay(0, 1)
    relay(1, 1)
    for q in (2, 4):
        for s in (1, 0):
            from_ring(q, 2, s)
    far_product(0, 0, 1)
    far_product(0, 0, 0)
    to_ring(10, 1, 1)
    far_product(1, 0, 1)
    to_ring(10, 1, 0)
    far_product(1, 0, 0)
    to_ring(11, 1, 1)
    to_ring(11, 1, 0)
    for q in (6, 8):
        for s in (1, 0):
            from_ring(q, 2, s)
    far_product(0, 1, 1)
    far_product(0, 1, 0)
    for q in (2, 3, 6, 7):
        to_owner(q)
    to_ring(12, 1, 1)
    far_product(1, 1, 1)
    to_ring(12, 1, 0)
    far_product(1, 1, 0)
    for q in (4, 5, 8, 9):
        to_owner(q)
    to_ring(13, 1, 1)
    to_ring(13, 1, 0)
    for q in (10, 11, 12, 13):
        for s in (1, 0):
            from_ring(q, 1, s)
            to_owner(q, lanes[s])
    arrived("owner", r3)
    totals = []
    for h in range(2):
        total = psum[h]
        for d in (1, 3, 2):
            for p in range(2):
                q = NUMBER[p, d, h]
                total += r3[q - 2]
        totals.append(total)

    left = -jnp.concatenate(totals, axis=0)
    for j in range(7, -1, -1):
        high, low = split(left[:, j * BLK : (j + 1) * BLK])
        width = (j + 1) * BLK
        both = dot(jnp.concatenate([high, low], axis=0), gsplit[0, j, :, :width])
        step = both[:32] + both[32:] + dot(high, gsplit[1, j, :, :width])
        xs[j] = step[:, j * BLK :].reshape(2, QUARTER, BLK)
        if j:
            left = left[:, : j * BLK] - step[:, : j * BLK]

    own = aligned(core * 64 + x * QUARTER, QUARTER, QUARTER)
    obuf[:, own, :] = xs[row]
    for i in range(4):
        for j in range(2):
            if (i, j) != (0, 0):
                target = where(dx=i, dc=j)
                copy(xs.at[target[0]], obuf.at[:, own, :], target, "spread", "spread")
    arrived("spread", xs.at[pl.ds(0, 7)])
    out[...] = obuf[...].reshape(COLS, BLK).T
    gone("shards", wrow.at[0, pl.ds(0, 3)])
    gone("rows", wrow.at[pl.ds(0, 3)])
    gone("blocks", gfull.at[pl.ds(0, 7)])
    for p in range(2):
        gone(("panel", p), lbuf.at[p, pl.ds(0, 3), pl.ds(0, LEN[p]), :])
        gone(("near", p), tbuf.at[p, pl.ds(1, 2), :, :, pl.ds(0, LEN[p]), :])
        gone(("hop", p), fwd.at[p, :, :, :, pl.ds(0, LEN[p]), :])
        gone(("far", p), tbuf.at[p, SLOT[2], :, :, pl.ds(0, LEN[p]), :])
    gone("pair", r1)
    gone("ring", ring)
    gone("owner", r3)
    gone("spread", xs.at[pl.ds(0, 7)])
    assert len(received) == RECEIVED and len(sending) == SENDING


def per_device(tail_vectors, lower_panel, window_rhs, window_block):
    anywhere = pl.BlockSpec(memory_space=pl.ANY)
    count = len(CHUNKS)
    return pl.pallas_call(
        kernel,
        name="window_solve",
        out_shape=jax.ShapeDtypeStruct((BLK, COLS), F32),
        in_specs=[anywhere] * 4,
        out_specs=pl.BlockSpec(memory_space=pltpu.VMEM),
        scratch_shapes=[
            pltpu.VMEM((2, 4, 2, 4, PART, BLK), F32),
            pltpu.VMEM((2, 2, 2, 2, PART, BLK), F32),
            pltpu.VMEM((2, 4, PART, WIN), F32),
            pltpu.VMEM((2, 2 * DEEP, WIN), BF16),
            pltpu.VMEM((2, COLS, 2 * DEEP), BF16),
            pltpu.VMEM((count, BLK, WIN), F32),
            pltpu.VMEM((4, 4, 8, WIN), F32),
            pltpu.VMEM((8, BLK, WIN), F32),
            pltpu.VMEM((2, 8, BLK, WIN), BF16),
            pltpu.VMEM((BLK, COLS), F32),
            pltpu.VMEM((count, 64, WIN), F32),
            pltpu.VMEM((count, 4, QUARTER, WIN), F32),
            pltpu.VMEM((count, 3, QUARTER, WIN), F32),
            pltpu.VMEM((count, QUARTER, WIN), F32),
            pltpu.VMEM((count - 2, QUARTER, WIN), F32),
            pltpu.VMEM((8, 2, QUARTER, BLK), F32),
            pltpu.VMEM((2, BLK, BLK), F32),
            pltpu.SemaphoreType.DMA((SENDING,)),
            pltpu.SemaphoreType.DMA((RECEIVED,)),
            pltpu.SemaphoreType.DMA((LOCAL,)),
        ],
        compiler_params=pltpu.CompilerParams(
            collective_id=0, has_side_effects=True, vmem_limit_bytes=62 * 1024 * 1024
        ),
    )(tail_vectors.reshape(4, 4, SEG, COLS), lower_panel, window_rhs, window_block)


def solution(mesh):
    in_specs = (P("row", "col"), P(("row", "col"), None), P("row", "col"), P(("row", "col"), None))
    return jax.shard_map(
        per_device, mesh=mesh, in_specs=in_specs, out_specs=P("row", "col"), check_vma=False
    )
```

```python
import jax
import jax.numpy as jnp
from jax import lax
from jax.experimental import pallas as pl
from jax.experimental.pallas import tpu as pltpu
from jax.sharding import PartitionSpec as P

F32, BF16 = jnp.float32, jnp.bfloat16
HIGHEST = lax.Precision.HIGHEST
SEG = 504
LEN = (256, 248)
PART = 256
DEEP = 4 * PART
WIN = 1024
COLS = 256
BLK = 128
QUARTER = 16
CHUNKS = [(None, 0, 0), (None, 0, 1)] + [(p, d, h) for near in ((1, 3), (2,)) for h in range(2) for p in range(2) for d in near]
NUMBER = {chunk: q for q, chunk in enumerate(CHUNKS)}
SLOT = (0, 1, 3, 2)
RECEIVED, SENDING, LOCAL = 62, 15, 8


def split(value):
    high = value.astype(BF16)
    return high, (value - high.astype(F32)).astype(BF16)


def dot(a, b, precision=None):
    return jnp.dot(a, b, preferred_element_type=F32, precision=precision)


def aligned(start, size, unit):
    return pl.ds(pl.multiple_of(start, unit), size)


def kernel(
    tail, panel, rhs, block, out,
    tbuf, fwd, lbuf, lsplit, tt, cbuf, wrow, gfull, gsplit, rhs_in,
    r1, part, ring, psum, r3, xs, obuf,
    send_sem, recv_sem, local_sem,
):
    row, col = lax.axis_index("row"), lax.axis_index("col")
    x, core = row // 2, row % 2
    z, y = col // 4, col % 4

    def where(dx=0, dc=0, dz=0, dy=0):
        new_row = 2 * ((x + dx + 4) % 4) + (core + dc) % 2
        new_col = 4 * ((z + dz + 4) % 4) + (y + dy + 4) % 4
        return (new_row, new_col)

    def along(p, step):
        return where(dy=step) if p == 0 else where(dz=step)

    def across(p, step):
        return along(1 - p, step)

    place = (z, y)

    received, sending = {}, {}

    def copy(src, dst, target, group, sent):
        at, out_at = received.setdefault(group, len(received)), sending.setdefault(sent, len(sending))
        pltpu.make_async_remote_copy(
            src_ref=src,
            dst_ref=dst,
            send_sem=send_sem.at[out_at],
            recv_sem=recv_sem.at[at],
            device_id=target,
            device_id_type=pl.DeviceIdType.MESH,
        ).start()

    def arrived(group, ref):
        pltpu.make_async_copy(ref, ref, recv_sem.at[received[group]]).wait()

    def gone(sent, ref):
        pltpu.make_async_copy(ref, ref, send_sem.at[sending[sent]]).wait()

    local = []

    def bring(src, dst):
        made = pltpu.make_async_copy(src, dst, local_sem.at[len(local)])
        made.start()
        local.append(made)
        return made

    def piece(p, step, h):
        columns = pl.ds(h * BLK, BLK)
        if p == 0:
            return tail.at[:, (y + step) % 4, pl.ds(0, LEN[0]), columns]
        return tail.at[(z + step) % 4, :, pl.ds(LEN[0], LEN[1]), columns]

    def landing(p, d, h):
        return tbuf.at[p, SLOT[d], h, :, pl.ds(0, LEN[p]), :]

    partners = [where(dy=i) for i in (1, 2, 3)] + [where(dz=i) for i in (1, 2, 3)]
    partners += [where(dx=i, dc=j) for i in range(4) for j in range(2) if (i, j) != (0, 0)]
    barrier = pltpu.get_barrier_semaphore()
    for partner in partners:
        pl.semaphore_signal(barrier, inc=1, device_id=partner, device_id_type=pl.DeviceIdType.MESH)
    pl.semaphore_wait(barrier, len(partners))

    lanes = pl.ds(0, WIN // 2), pl.ds(WIN // 2, WIN // 2)
    for i in (1, 3, 2):
        copy(block, wrow.at[z, y], where(dy=i), "shards", "shards")

    def half(p, side):
        return pl.ds(0, 128) if side == 0 else pl.ds(128, LEN[p] - 128)

    def send_panel(p, step, side, group):
        src = pl.ds(p * PART + half(p, side).start, half(p, side).size)
        copy(panel.at[src, :], lbuf.at[p, place[p], half(p, side), :], across(p, step), group, ("panel", p))

    for p in (1, 0):
        send_panel(p, 1, 0, ("up", p))
        send_panel(p, 3, 1, ("down", p))
    own_block = bring(block, wrow.at[z, y])
    own_panel = [
        bring(panel.at[pl.ds(p * PART, LEN[p]), :], lbuf.at[p, place[p], pl.ds(0, LEN[p]), :]) for p in range(2)
    ]
    own_rhs = bring(rhs, rhs_in)
    own_tail = [bring(piece(p, 0, h), landing(p, 0, h)) for p in range(2) for h in range(2)]

    for i in range(4):
        lbuf[1, i, LEN[1] :, :] = jnp.zeros((PART - LEN[1], WIN), F32)
        for d in range(4):
            for h in range(2):
                tbuf[1, d, h, i, LEN[1] :, :] = jnp.zeros((PART - LEN[1], BLK), F32)

    own_block.wait()
    arrived("shards", wrow.at[0, pl.ds(0, 3)])
    for i in (1, 3, 2):
        copy(wrow.at[z], wrow.at[z], where(dz=i), "rows", "rows")
    for p in (1, 0):
        send_panel(p, 1, 1, ("second", p))
        send_panel(p, 3, 0, ("second", p))

    for p in (1, 0):
        for name, step, side in (("up", 1, 0), ("down", 3, 1)):
            at = lbuf.at[p, (place[p] - step + 4) % 4, half(p, side), :]
            arrived((name, p), at)
            copy(at, at, across(p, step), ("onward", p), ("panel", p))

    for p, d, h in CHUNKS[2:10]:
        copy(piece(p, d, h), landing(p, d, h), along(p, d), ("near", p, h), ("near", p))
    for h in range(2):
        for i in range(2):
            for p in range(2):
                side, columns = pl.ds(2 * i, 2), pl.ds(h * BLK, BLK)
                if p == 0:
                    src = tail.at[side, (y + 2) % 4, pl.ds(0, LEN[0]), columns]
                else:
                    src = tail.at[(z + 2) % 4, side, pl.ds(LEN[0], LEN[1]), columns]
                dst = fwd.at[p, h, i, :, pl.ds(0, LEN[p]), :]
                copy(src, dst, along(p, 1 + 2 * i), ("hop", p, h), ("hop", p))

    def relay(p, h):
        arrived(("hop", p, h), fwd.at[p, h, :, :, pl.ds(0, LEN[p]), :])
        for i in range(2):
            src = fwd.at[p, h, i, :, pl.ds(0, LEN[p]), :]
            dst = tbuf.at[p, SLOT[2], h, pl.ds(2 * i, 2), pl.ds(0, LEN[p]), :]
            copy(src, dst, along(p, 1 + 2 * i), ("far", p, h), ("far", p))

    arrived("rows", wrow.at[pl.ds(0, 3)])

    rows = lax.broadcasted_iota(jnp.int32, (BLK, BLK), 0)
    cols = lax.broadcasted_iota(jnp.int32, (BLK, BLK), 1)
    eye = jnp.where(rows == cols, 1.0, 0.0).astype(F32)
    own_cols = aligned(row * BLK, BLK, BLK)
    diagonal = wrow[:, :, :, own_cols].reshape(BLK, BLK)
    on_diag = jnp.where(rows == cols, diagonal, 0.0)
    diag_rows = jnp.sum(on_diag, axis=1, keepdims=True)
    diag_cols = jnp.sum(on_diag, axis=0, keepdims=True)
    lower = jnp.where(rows > cols, diagonal, 0.0) / diag_rows
    inverse, power = eye - lower, dot(lower, lower, HIGHEST)
    for _ in range(6):
        both = dot(jnp.concatenate([inverse, power], axis=0), power, HIGHEST)
        inverse, power = inverse + both[:BLK], both[BLK:]
    inverse = inverse / diag_cols
    gfull[row] = dot(inverse, wrow[...].reshape(BLK, WIN), HIGHEST)
    gfull[row, :, own_cols] = inverse
    for i in (1, 3, 2):
        copy(gfull.at[row], gfull.at[row], where(dx=i), "over_x", "blocks")
    copy(gfull.at[row], gfull.at[row], where(dc=1), "to_other", "blocks")

    def split_panel(p, slot):
        @pl.loop(0, 2)
        def _(step):
            high, low = split(lbuf[p, slot, aligned(step * BLK, BLK, BLK), :])
            lsplit[p, aligned(slot * PART + step * BLK, BLK, BLK), :] = low
            lsplit[p, aligned(DEEP + slot * PART + step * BLK, BLK, BLK), :] = high

    def turn(p, i, d, h, slots):
        @pl.loop(*slots)
        def _(step):
            high, low = split(tbuf[p, SLOT[d], h, step].T)
            tt[p, pl.ds(i * BLK, BLK), aligned(step * PART, PART, PART)] = high
            tt[p, pl.ds(i * BLK, BLK), aligned(DEEP + step * PART, PART, PART)] = low

    def add_own(p, slot):
        high_at, low_at = aligned(slot * PART, PART, PART), aligned(DEEP + slot * PART, PART, PART)

        @pl.loop(0, 4)
        def _(step):
            at = aligned(step * 256, 256, 256)
            value = dot(tt[p, :, low_at], lsplit[p, low_at, at]) + dot(tt[p, :, high_at], lsplit[p, high_at, at])
            value += dot(tt[p, :, high_at], lsplit[p, low_at, at])
            cbuf[0, :, at] += value[:BLK]
            cbuf[1, :, at] += value[BLK:]

    for made in own_panel + own_tail:
        made.wait()
    own_rhs.wait()
    turned = rhs_in[...].T
    for h in range(2):
        cbuf[h] = jnp.zeros((BLK, WIN), F32)
        cbuf[h, :, own_cols] = -turned[h * BLK : (h + 1) * BLK]
    for p in range(2):
        split_panel(p, place[p])
        for h in range(2):
            turn(p, h, 0, h, (0, 4))
    for p in (1, 0):
        arrived(("second", p), lbuf.at[p, 0, pl.ds(0, LEN[p]), :])
        split_panel(p, (place[p] + 3) % 4)
        split_panel(p, (place[p] + 1) % 4)

        @pl.loop(0, 3)
        def _(i):
            add_own(p, (place[p] + 3 + i) % 4)

    for p in (1, 0):
        arrived(("onward", p), lbuf.at[p, 0, pl.ds(0, LEN[p]), :])
        split_panel(p, (place[p] + 2) % 4)
        add_own(p, (place[p] + 2) % 4)

    keep, give = aligned(core * 64, 64, 64), aligned((1 - core) * 64, 64, 64)

    def to_pair(q, n, s):
        at = pl.ds(q, n)
        copy(cbuf.at[at, give, lanes[s]], r1.at[at, :, lanes[s]], where(dc=1), ("pair", q, s), "pair")

    def to_ring(q, n, s):
        at = pl.ds(q, n)
        arrived(("pair", q, s), r1.at[at, :, lanes[s]])
        value = cbuf[at, keep, lanes[s]] + r1[at, :, lanes[s]]
        part[at, :, :, lanes[s]] = value.reshape(n, 4, QUARTER, WIN // 2)
        for i in (2, 1, 3):
            src, dst = part.at[at, (x + i) % 4, :, lanes[s]], ring.at[at, i - 1, :, lanes[s]]
            copy(src, dst, where(dx=i), ("ring", q, s), "ring")

    def from_ring(q, n, s):
        arrived(("ring", q, s), ring.at[pl.ds(q, n), :, :, lanes[s]])
        at = lanes[s]
        for k in range(q, q + n):
            psum[k, :, at] = part[k, x, :, at] + ring[k, 0, :, at] + ring[k, 1, :, at] + ring[k, 2, :, at]

    def to_owner(q, at=pl.ds(0, WIN)):
        p, d, _ = CHUNKS[q]
        copy(psum.at[q, :, at], r3.at[q - 2, :, at], along(p, -d), "owner", "owner")

    def near_product(p, h, s):
        if s:
            arrived(("near", p, h), tbuf.at[p, pl.ds(1, 2), h, :, pl.ds(0, LEN[p]), :])
            for i, d in enumerate((1, 3)):
                turn(p, i, d, h, (0, 4))
        q = NUMBER[p, 1, h]

        @pl.loop(2 * s, 2 * s + 2)
        def _(step):
            at = aligned(step * 256, 256, 256)
            value = dot(tt[p], lsplit[p, :, at]) + dot(tt[p, :, :DEEP], lsplit[p, DEEP:, at])
            for i in range(2):
                cbuf[q + i, :, at] = value[i * BLK : (i + 1) * BLK]

        to_pair(q, 2, s)

    def far_product(p, h, s):
        if s:
            arrived(("far", p, h), landing(p, 2, h))

            @pl.loop(0, 4)
            def _(step):
                high, low = split(tbuf[p, SLOT[2], h, step].T)
                tt[p, pl.ds(0, BLK), aligned(step * PART, PART, PART)] = high
                tt[p, pl.ds(BLK, BLK), aligned(step * PART, PART, PART)] = low

        q = NUMBER[p, 2, h]

        @pl.loop(2 * s, 2 * s + 2)
        def _(step):
            at = aligned(step * 256, 256, 256)
            both = dot(tt[p, :, :DEEP], lsplit[p, DEEP:, at])
            cbuf[q, :, at] = both[:BLK] + both[BLK:] + dot(tt[p, :BLK, :DEEP], lsplit[p, :DEEP, at])

        to_pair(q, 1, s)

    to_pair(0, 2, 1)
    to_pair(0, 2, 0)
    to_ring(0, 2, 1)
    to_ring(0, 2, 0)
    near_product(0, 0, 1)
    near_product(0, 0, 0)
    to_ring(2, 2, 1)
    near_product(1, 0, 1)
    to_ring(2, 2, 0)
    near_product(1, 0, 0)
    to_ring(4, 2, 1)
    arrived("over_x", gfull.at[pl.ds(0, 3)])
    for i in (1, 3, 2):
        slot = 2 * ((x - i + 4) % 4) + core
        copy(gfull.at[slot], gfull.at[slot], where(dc=1), "to_other", "blocks")
    to_ring(4, 2, 0)
    from_ring(0, 2, 1)
    from_ring(0, 2, 0)
    near_product(0, 1, 1)
    near_product(0, 1, 0)
    to_ring(6, 2, 1)
    near_product(1, 1, 1)
    to_ring(6, 2, 0)
    near_product(1, 1, 0)
    to_ring(8, 2, 1)
    relay(0, 0)
    relay(1, 0)
    to_ring(8, 2, 0)
    arrived("to_other", gfull.at[pl.ds(0, 4)])

    @pl.loop(0, 8)
    def _(step):
        high, low = split(gfull[step])
        gsplit[0, step] = high
        gsplit[1, step] = low

    relay(0, 1)
    relay(1, 1)
    for q in (2, 4):
        for s in (1, 0):
            from_ring(q, 2, s)
    far_product(0, 0, 1)
    far_product(0, 0, 0)
    to_ring(10, 1, 1)
    to_ring(10, 1, 0)
    far_product(1, 0, 1)
    far_product(1, 0, 0)
    to_ring(11, 1, 1)
    far_product(0, 1, 1)
    to_ring(11, 1, 0)
    far_product(0, 1, 0)
    to_ring(12, 1, 1)
    far_product(1, 1, 1)
    to_ring(12, 1, 0)
    far_product(1, 1, 0)
    to_ring(13, 1, 1)
    for q in (6, 8):
        for s in (1, 0):
            from_ring(q, 2, s)
    for q in (2, 3, 6, 7):
        to_owner(q)
    to_ring(13, 1, 0)
    for q in (4, 5, 8, 9):
        to_owner(q)
    for q in (10, 11, 12, 13):
        for s in (1, 0):
            from_ring(q, 1, s)
            to_owner(q, lanes[s])
    arrived("owner", r3)
    totals = []
    for h in range(2):
        total = psum[h]
        for d in (1, 3, 2):
            for p in range(2):
                q = NUMBER[p, d, h]
                total += r3[q - 2]
        totals.append(total)

    left = -jnp.concatenate(totals, axis=0)
    for j in range(7, -1, -1):
        high, low = split(left[:, j * BLK : (j + 1) * BLK])
        width = (j + 1) * BLK
        both = dot(jnp.concatenate([high, low], axis=0), gsplit[0, j, :, :width])
        step = both[:32] + both[32:] + dot(high, gsplit[1, j, :, :width])
        xs[j] = step[:, j * BLK :].reshape(2, QUARTER, BLK)
        if j:
            left = left[:, : j * BLK] - step[:, : j * BLK]

    own = aligned(core * 64 + x * QUARTER, QUARTER, QUARTER)
    obuf[:, own, :] = xs[row]
    for i in range(4):
        for j in range(2):
            if (i, j) != (0, 0):
                target = where(dx=i, dc=j)
                copy(xs.at[target[0]], obuf.at[:, own, :], target, "spread", "spread")
    arrived("spread", xs.at[pl.ds(0, 7)])
    out[...] = obuf[...].reshape(COLS, BLK).T
    gone("shards", wrow.at[0, pl.ds(0, 3)])
    gone("rows", wrow.at[pl.ds(0, 3)])
    gone("blocks", gfull.at[pl.ds(0, 7)])
    for p in range(2):
        gone(("panel", p), lbuf.at[p, pl.ds(0, 3), pl.ds(0, LEN[p]), :])
        gone(("near", p), tbuf.at[p, pl.ds(1, 2), :, :, pl.ds(0, LEN[p]), :])
        gone(("hop", p), fwd.at[p, :, :, :, pl.ds(0, LEN[p]), :])
        gone(("far", p), tbuf.at[p, SLOT[2], :, :, pl.ds(0, LEN[p]), :])
    gone("pair", r1)
    gone("ring", ring)
    gone("owner", r3)
    gone("spread", xs.at[pl.ds(0, 7)])
    assert len(received) == RECEIVED and len(sending) == SENDING


def per_device(tail_vectors, lower_panel, window_rhs, window_block):
    anywhere = pl.BlockSpec(memory_space=pl.ANY)
    count = len(CHUNKS)
    return pl.pallas_call(
        kernel,
        name="window_solve",
        out_shape=jax.ShapeDtypeStruct((BLK, COLS), F32),
        in_specs=[anywhere] * 4,
        out_specs=pl.BlockSpec(memory_space=pltpu.VMEM),
        scratch_shapes=[
            pltpu.VMEM((2, 4, 2, 4, PART, BLK), F32),
            pltpu.VMEM((2, 2, 2, 2, PART, BLK), F32),
            pltpu.VMEM((2, 4, PART, WIN), F32),
            pltpu.VMEM((2, 2 * DEEP, WIN), BF16),
            pltpu.VMEM((2, COLS, 2 * DEEP), BF16),
            pltpu.VMEM((count, BLK, WIN), F32),
            pltpu.VMEM((4, 4, 8, WIN), F32),
            pltpu.VMEM((8, BLK, WIN), F32),
            pltpu.VMEM((2, 8, BLK, WIN), BF16),
            pltpu.VMEM((BLK, COLS), F32),
            pltpu.VMEM((count, 64, WIN), F32),
            pltpu.VMEM((count, 4, QUARTER, WIN), F32),
            pltpu.VMEM((count, 3, QUARTER, WIN), F32),
            pltpu.VMEM((count, QUARTER, WIN), F32),
            pltpu.VMEM((count - 2, QUARTER, WIN), F32),
            pltpu.VMEM((8, 2, QUARTER, BLK), F32),
            pltpu.VMEM((2, BLK, BLK), F32),
            pltpu.SemaphoreType.DMA((SENDING,)),
            pltpu.SemaphoreType.DMA((RECEIVED,)),
            pltpu.SemaphoreType.DMA((LOCAL,)),
        ],
        compiler_params=pltpu.CompilerParams(
            collective_id=0, has_side_effects=True, vmem_limit_bytes=62 * 1024 * 1024
        ),
    )(tail_vectors.reshape(4, 4, SEG, COLS), lower_panel, window_rhs, window_block)


def solution(mesh):
    in_specs = (P("row", "col"), P(("row", "col"), None), P("row", "col"), P(("row", "col"), None))
    return jax.shard_map(
        per_device, mesh=mesh, in_specs=in_specs, out_specs=P("row", "col"), check_vma=False
    )
```

```python
import jax
import jax.numpy as jnp
from jax import lax
from jax.experimental import pallas as pl
from jax.experimental.pallas import tpu as pltpu
from jax.sharding import PartitionSpec as P

F32, BF16 = jnp.float32, jnp.bfloat16
HIGHEST = lax.Precision.HIGHEST
SEG = 504
LEN = (256, 248)
PART = 256
DEEP = 4 * PART
WIN = 1024
COLS = 256
BLK = 128
QUARTER = 16
CHUNKS = [(None, 0, 0), (None, 0, 1)] + [(p, d, h) for near in ((1, 3), (2,)) for h in range(2) for p in range(2) for d in near]
NUMBER = {chunk: q for q, chunk in enumerate(CHUNKS)}
SLOT = (0, 1, 3, 2)
RECEIVED, SENDING, LOCAL = 62, 15, 8


def split(value):
    high = value.astype(BF16)
    return high, (value - high.astype(F32)).astype(BF16)


def dot(a, b, precision=None):
    return jnp.dot(a, b, preferred_element_type=F32, precision=precision)


def aligned(start, size, unit):
    return pl.ds(pl.multiple_of(start, unit), size)


def kernel(
    tail, panel, rhs, block, out,
    tbuf, fwd, lbuf, lsplit, tt, cbuf, wrow, gfull, gsplit, rhs_in,
    r1, part, ring, psum, r3, xs, obuf,
    send_sem, recv_sem, local_sem,
):
    row, col = lax.axis_index("row"), lax.axis_index("col")
    x, core = row // 2, row % 2
    z, y = col // 4, col % 4

    def where(dx=0, dc=0, dz=0, dy=0):
        new_row = 2 * ((x + dx + 4) % 4) + (core + dc) % 2
        new_col = 4 * ((z + dz + 4) % 4) + (y + dy + 4) % 4
        return (new_row, new_col)

    def along(p, step):
        return where(dy=step) if p == 0 else where(dz=step)

    def across(p, step):
        return along(1 - p, step)

    place = (z, y)

    received, sending = {}, {}

    def copy(src, dst, target, group, sent):
        at, out_at = received.setdefault(group, len(received)), sending.setdefault(sent, len(sending))
        pltpu.make_async_remote_copy(
            src_ref=src,
            dst_ref=dst,
            send_sem=send_sem.at[out_at],
            recv_sem=recv_sem.at[at],
            device_id=target,
            device_id_type=pl.DeviceIdType.MESH,
        ).start()

    def arrived(group, ref):
        pltpu.make_async_copy(ref, ref, recv_sem.at[received[group]]).wait()

    def gone(sent, ref):
        pltpu.make_async_copy(ref, ref, send_sem.at[sending[sent]]).wait()

    local = []

    def bring(src, dst):
        made = pltpu.make_async_copy(src, dst, local_sem.at[len(local)])
        made.start()
        local.append(made)
        return made

    def piece(p, step, h):
        columns = pl.ds(h * BLK, BLK)
        if p == 0:
            return tail.at[:, (y + step) % 4, pl.ds(0, LEN[0]), columns]
        return tail.at[(z + step) % 4, :, pl.ds(LEN[0], LEN[1]), columns]

    def landing(p, d, h):
        return tbuf.at[p, SLOT[d], h, :, pl.ds(0, LEN[p]), :]

    partners = [where(dy=i) for i in (1, 2, 3)] + [where(dz=i) for i in (1, 2, 3)]
    partners += [where(dx=i, dc=j) for i in range(4) for j in range(2) if (i, j) != (0, 0)]
    barrier = pltpu.get_barrier_semaphore()
    for partner in partners:
        pl.semaphore_signal(barrier, inc=1, device_id=partner, device_id_type=pl.DeviceIdType.MESH)
    pl.semaphore_wait(barrier, len(partners))

    lanes = pl.ds(0, WIN // 2), pl.ds(WIN // 2, WIN // 2)
    for i in (1, 3, 2):
        copy(block, wrow.at[z, y], where(dy=i), "shards", "shards")

    def half(p, side):
        return pl.ds(0, 128) if side == 0 else pl.ds(128, LEN[p] - 128)

    def send_panel(p, step, side, group):
        src = pl.ds(p * PART + half(p, side).start, half(p, side).size)
        copy(panel.at[src, :], lbuf.at[p, place[p], half(p, side), :], across(p, step), group, ("panel", p))

    for p in (1, 0):
        send_panel(p, 1, 0, ("up", p))
        send_panel(p, 3, 1, ("down", p))
    own_block = bring(block, wrow.at[z, y])
    own_panel = [
        bring(panel.at[pl.ds(p * PART, LEN[p]), :], lbuf.at[p, place[p], pl.ds(0, LEN[p]), :]) for p in range(2)
    ]
    own_rhs = bring(rhs, rhs_in)
    own_tail = [bring(piece(p, 0, h), landing(p, 0, h)) for p in range(2) for h in range(2)]

    for i in range(4):
        lbuf[1, i, LEN[1] :, :] = jnp.zeros((PART - LEN[1], WIN), F32)
        for d in range(4):
            for h in range(2):
                tbuf[1, d, h, i, LEN[1] :, :] = jnp.zeros((PART - LEN[1], BLK), F32)

    own_block.wait()
    arrived("shards", wrow.at[0, pl.ds(0, 3)])
    for i in (1, 3, 2):
        copy(wrow.at[z], wrow.at[z], where(dz=i), "rows", "rows")
    for p in (1, 0):
        send_panel(p, 1, 1, ("second", p))
        send_panel(p, 3, 0, ("second", p))

    for p in (1, 0):
        for name, step, side in (("up", 1, 0), ("down", 3, 1)):
            at = lbuf.at[p, (place[p] - step + 4) % 4, half(p, side), :]
            arrived((name, p), at)
            copy(at, at, across(p, step), ("onward", p), ("panel", p))

    for p, d, h in CHUNKS[2:10]:
        copy(piece(p, d, h), landing(p, d, h), along(p, d), ("near", p, h), ("near", p))
    for h in range(2):
        for i in range(2):
            for p in range(2):
                side, columns = pl.ds(2 * i, 2), pl.ds(h * BLK, BLK)
                if p == 0:
                    src = tail.at[side, (y + 2) % 4, pl.ds(0, LEN[0]), columns]
                else:
                    src = tail.at[(z + 2) % 4, side, pl.ds(LEN[0], LEN[1]), columns]
                dst = fwd.at[p, h, i, :, pl.ds(0, LEN[p]), :]
                copy(src, dst, along(p, 1 + 2 * i), ("hop", p, h), ("hop", p))

    def relay(p, h):
        arrived(("hop", p, h), fwd.at[p, h, :, :, pl.ds(0, LEN[p]), :])
        for i in range(2):
            src = fwd.at[p, h, i, :, pl.ds(0, LEN[p]), :]
            dst = tbuf.at[p, SLOT[2], h, pl.ds(2 * i, 2), pl.ds(0, LEN[p]), :]
            copy(src, dst, along(p, 1 + 2 * i), ("far", p, h), ("far", p))

    arrived("rows", wrow.at[pl.ds(0, 3)])

    rows = lax.broadcasted_iota(jnp.int32, (BLK, BLK), 0)
    cols = lax.broadcasted_iota(jnp.int32, (BLK, BLK), 1)
    eye = jnp.where(rows == cols, 1.0, 0.0).astype(F32)
    own_cols = aligned(row * BLK, BLK, BLK)
    diagonal = wrow[:, :, :, own_cols].reshape(BLK, BLK)
    on_diag = jnp.where(rows == cols, diagonal, 0.0)
    diag_rows = jnp.sum(on_diag, axis=1, keepdims=True)
    diag_cols = jnp.sum(on_diag, axis=0, keepdims=True)
    lower = jnp.where(rows > cols, diagonal, 0.0) / diag_rows
    inverse, power = eye - lower, dot(lower, lower, HIGHEST)
    for _ in range(6):
        both = dot(jnp.concatenate([inverse, power], axis=0), power, HIGHEST)
        inverse, power = inverse + both[:BLK], both[BLK:]
    inverse = inverse / diag_cols
    gfull[row] = dot(inverse, wrow[...].reshape(BLK, WIN), HIGHEST)
    gfull[row, :, own_cols] = inverse
    for i in (1, 3, 2):
        copy(gfull.at[row], gfull.at[row], where(dx=i), "over_x", "blocks")
    copy(gfull.at[row], gfull.at[row], where(dc=1), "to_other", "blocks")

    def split_panel(p, slot):
        @pl.loop(0, 2)
        def _(step):
            high, low = split(lbuf[p, slot, aligned(step * BLK, BLK, BLK), :])
            lsplit[p, aligned(slot * PART + step * BLK, BLK, BLK), :] = low
            lsplit[p, aligned(DEEP + slot * PART + step * BLK, BLK, BLK), :] = high

    def turn(p, i, d, h, slots):
        @pl.loop(*slots)
        def _(step):
            high, low = split(tbuf[p, SLOT[d], h, step].T)
            tt[p, pl.ds(i * BLK, BLK), aligned(step * PART, PART, PART)] = high
            tt[p, pl.ds(i * BLK, BLK), aligned(DEEP + step * PART, PART, PART)] = low

    def add_own(p, slot):
        high_at, low_at = aligned(slot * PART, PART, PART), aligned(DEEP + slot * PART, PART, PART)

        @pl.loop(0, 4)
        def _(step):
            at = aligned(step * 256, 256, 256)
            value = dot(tt[p, :, low_at], lsplit[p, low_at, at]) + dot(tt[p, :, high_at], lsplit[p, high_at, at])
            value += dot(tt[p, :, high_at], lsplit[p, low_at, at])
            cbuf[0, :, at] += value[:BLK]
            cbuf[1, :, at] += value[BLK:]

    for made in own_panel + own_tail:
        made.wait()
    own_rhs.wait()
    turned = rhs_in[...].T
    for h in range(2):
        cbuf[h] = jnp.zeros((BLK, WIN), F32)
        cbuf[h, :, own_cols] = -turned[h * BLK : (h + 1) * BLK]
    for p in range(2):
        split_panel(p, place[p])
        for h in range(2):
            turn(p, h, 0, h, (0, 4))
    for p in (1, 0):
        arrived(("second", p), lbuf.at[p, 0, pl.ds(0, LEN[p]), :])
        split_panel(p, (place[p] + 3) % 4)
        split_panel(p, (place[p] + 1) % 4)

        @pl.loop(0, 3)
        def _(i):
            add_own(p, (place[p] + 3 + i) % 4)

    for p in (1, 0):
        arrived(("onward", p), lbuf.at[p, 0, pl.ds(0, LEN[p]), :])
        split_panel(p, (place[p] + 2) % 4)
        add_own(p, (place[p] + 2) % 4)

    keep, give = aligned(core * 64, 64, 64), aligned((1 - core) * 64, 64, 64)

    def to_pair(q, n, s):
        at = pl.ds(q, n)
        copy(cbuf.at[at, give, lanes[s]], r1.at[at, :, lanes[s]], where(dc=1), ("pair", q, s), "pair")

    def to_ring(q, n, s):
        at = pl.ds(q, n)
        arrived(("pair", q, s), r1.at[at, :, lanes[s]])
        value = cbuf[at, keep, lanes[s]] + r1[at, :, lanes[s]]
        part[at, :, :, lanes[s]] = value.reshape(n, 4, QUARTER, WIN // 2)
        for i in (2, 1, 3):
            src, dst = part.at[at, (x + i) % 4, :, lanes[s]], ring.at[at, i - 1, :, lanes[s]]
            copy(src, dst, where(dx=i), ("ring", q, s), "ring")

    def from_ring(q, n, s):
        arrived(("ring", q, s), ring.at[pl.ds(q, n), :, :, lanes[s]])
        at = lanes[s]
        for k in range(q, q + n):
            psum[k, :, at] = part[k, x, :, at] + ring[k, 0, :, at] + ring[k, 1, :, at] + ring[k, 2, :, at]

    def to_owner(q, at=pl.ds(0, WIN)):
        p, d, _ = CHUNKS[q]
        copy(psum.at[q, :, at], r3.at[q - 2, :, at], along(p, -d), "owner", "owner")

    def near_product(p, h, s):
        if s:
            arrived(("near", p, h), tbuf.at[p, pl.ds(1, 2), h, :, pl.ds(0, LEN[p]), :])
            for i, d in enumerate((1, 3)):
                turn(p, i, d, h, (0, 4))
        q = NUMBER[p, 1, h]

        @pl.loop(2 * s, 2 * s + 2)
        def _(step):
            at = aligned(step * 256, 256, 256)
            value = dot(tt[p], lsplit[p, :, at]) + dot(tt[p, :, :DEEP], lsplit[p, DEEP:, at])
            for i in range(2):
                cbuf[q + i, :, at] = value[i * BLK : (i + 1) * BLK]

        to_pair(q, 2, s)

    def far_product(p, h, s):
        if s:
            arrived(("far", p, h), landing(p, 2, h))

            @pl.loop(0, 4)
            def _(step):
                high, low = split(tbuf[p, SLOT[2], h, step].T)
                tt[p, pl.ds(0, BLK), aligned(step * PART, PART, PART)] = high
                tt[p, pl.ds(BLK, BLK), aligned(step * PART, PART, PART)] = low

        q = NUMBER[p, 2, h]

        @pl.loop(2 * s, 2 * s + 2)
        def _(step):
            at = aligned(step * 256, 256, 256)
            both = dot(tt[p, :, :DEEP], lsplit[p, DEEP:, at])
            cbuf[q, :, at] = both[:BLK] + both[BLK:] + dot(tt[p, :BLK, :DEEP], lsplit[p, :DEEP, at])

        to_pair(q, 1, s)

    to_pair(0, 2, 1)
    to_pair(0, 2, 0)
    to_ring(0, 2, 1)
    to_ring(0, 2, 0)
    near_product(0, 0, 1)
    near_product(0, 0, 0)
    to_ring(2, 2, 1)
    near_product(1, 0, 1)
    to_ring(2, 2, 0)
    near_product(1, 0, 0)
    to_ring(4, 2, 1)
    arrived("over_x", gfull.at[pl.ds(0, 3)])
    for i in (1, 3, 2):
        slot = 2 * ((x - i + 4) % 4) + core
        copy(gfull.at[slot], gfull.at[slot], where(dc=1), "to_other", "blocks")
    to_ring(4, 2, 0)
    from_ring(0, 2, 1)
    from_ring(0, 2, 0)
    near_product(0, 1, 1)
    near_product(0, 1, 0)
    to_ring(6, 2, 1)
    near_product(1, 1, 1)
    to_ring(6, 2, 0)
    near_product(1, 1, 0)
    to_ring(8, 2, 1)
    relay(0, 0)
    relay(1, 0)
    to_ring(8, 2, 0)
    arrived("to_other", gfull.at[pl.ds(0, 4)])

    @pl.loop(0, 8)
    def _(step):
        high, low = split(gfull[step])
        gsplit[0, step] = high
        gsplit[1, step] = low

    relay(0, 1)
    relay(1, 1)
    for q in (2, 4):
        for s in (1, 0):
            from_ring(q, 2, s)
    far_product(0, 0, 1)
    far_product(0, 0, 0)
    to_ring(10, 1, 1)
    to_ring(10, 1, 0)
    far_product(1, 0, 1)
    far_product(1, 0, 0)
    to_ring(11, 1, 1)
    far_product(0, 1, 1)
    to_ring(11, 1, 0)
    far_product(0, 1, 0)
    to_ring(12, 1, 1)
    far_product(1, 1, 1)
    to_ring(12, 1, 0)
    far_product(1, 1, 0)
    to_ring(13, 1, 1)
    for q in (6, 8):
        for s in (1, 0):
            from_ring(q, 2, s)
    for q in (2, 3, 6, 7):
        to_owner(q)
    to_ring(13, 1, 0)
    for q in (4, 5, 8, 9):
        to_owner(q)
    for q in (10, 11, 12, 13):
        for s in (1, 0):
            from_ring(q, 1, s)
            to_owner(q, lanes[s])
    arrived("owner", r3)
    totals = []
    for h in range(2):
        total = psum[h]
        for d in (1, 3, 2):
            for p in range(2):
                q = NUMBER[p, d, h]
                total += r3[q - 2]
        totals.append(total)

    own = aligned(core * 64 + x * QUARTER, QUARTER, QUARTER)
    left = -jnp.concatenate(totals, axis=0)
    for j in range(7, -1, -1):
        high, low = split(left[:, j * BLK : (j + 1) * BLK])
        width = (j + 1) * BLK
        both = dot(jnp.concatenate([high, low], axis=0), gsplit[0, j, :, :width])
        step = both[:32] + both[32:] + dot(high, gsplit[1, j, :, :width])
        xs[j] = step[:, j * BLK :].reshape(2, QUARTER, BLK)

        @pl.when(row != j)
        def _():
            copy(xs.at[j], obuf.at[:, own, :], (j, col), "spread", "spread")

        if j:
            left = left[:, : j * BLK] - step[:, : j * BLK]

    obuf[:, own, :] = xs[row]
    arrived("spread", xs.at[pl.ds(0, 7)])
    out[...] = obuf[...].reshape(COLS, BLK).T
    gone("shards", wrow.at[0, pl.ds(0, 3)])
    gone("rows", wrow.at[pl.ds(0, 3)])
    gone("blocks", gfull.at[pl.ds(0, 7)])
    for p in range(2):
        gone(("panel", p), lbuf.at[p, pl.ds(0, 3), pl.ds(0, LEN[p]), :])
        gone(("near", p), tbuf.at[p, pl.ds(1, 2), :, :, pl.ds(0, LEN[p]), :])
        gone(("hop", p), fwd.at[p, :, :, :, pl.ds(0, LEN[p]), :])
        gone(("far", p), tbuf.at[p, SLOT[2], :, :, pl.ds(0, LEN[p]), :])
    gone("pair", r1)
    gone("ring", ring)
    gone("owner", r3)
    gone("spread", xs.at[pl.ds(0, 7)])
    assert len(received) == RECEIVED and len(sending) == SENDING


def per_device(tail_vectors, lower_panel, window_rhs, window_block):
    anywhere = pl.BlockSpec(memory_space=pl.ANY)
    count = len(CHUNKS)
    return pl.pallas_call(
        kernel,
        name="window_solve",
        out_shape=jax.ShapeDtypeStruct((BLK, COLS), F32),
        in_specs=[anywhere] * 4,
        out_specs=pl.BlockSpec(memory_space=pltpu.VMEM),
        scratch_shapes=[
            pltpu.VMEM((2, 4, 2, 4, PART, BLK), F32),
            pltpu.VMEM((2, 2, 2, 2, PART, BLK), F32),
            pltpu.VMEM((2, 4, PART, WIN), F32),
            pltpu.VMEM((2, 2 * DEEP, WIN), BF16),
            pltpu.VMEM((2, COLS, 2 * DEEP), BF16),
            pltpu.VMEM((count, BLK, WIN), F32),
            pltpu.VMEM((4, 4, 8, WIN), F32),
            pltpu.VMEM((8, BLK, WIN), F32),
            pltpu.VMEM((2, 8, BLK, WIN), BF16),
            pltpu.VMEM((BLK, COLS), F32),
            pltpu.VMEM((count, 64, WIN), F32),
            pltpu.VMEM((count, 4, QUARTER, WIN), F32),
            pltpu.VMEM((count, 3, QUARTER, WIN), F32),
            pltpu.VMEM((count, QUARTER, WIN), F32),
            pltpu.VMEM((count - 2, QUARTER, WIN), F32),
            pltpu.VMEM((8, 2, QUARTER, BLK), F32),
            pltpu.VMEM((2, BLK, BLK), F32),
            pltpu.SemaphoreType.DMA((SENDING,)),
            pltpu.SemaphoreType.DMA((RECEIVED,)),
            pltpu.SemaphoreType.DMA((LOCAL,)),
        ],
        compiler_params=pltpu.CompilerParams(
            collective_id=0, has_side_effects=True, vmem_limit_bytes=62 * 1024 * 1024
        ),
    )(tail_vectors.reshape(4, 4, SEG, COLS), lower_panel, window_rhs, window_block)


def solution(mesh):
    in_specs = (P("row", "col"), P(("row", "col"), None), P("row", "col"), P(("row", "col"), None))
    return jax.shard_map(
        per_device, mesh=mesh, in_specs=in_specs, out_specs=P("row", "col"), check_vma=False
    )
```

```python
import jax
import jax.numpy as jnp
from jax import lax
from jax.experimental import pallas as pl
from jax.experimental.pallas import tpu as pltpu
from jax.sharding import PartitionSpec as P

F32, BF16 = jnp.float32, jnp.bfloat16
HIGHEST = lax.Precision.HIGHEST
SEG = 504
LEN = (256, 248)
PART = 256
DEEP = 4 * PART
WIN = 1024
COLS = 256
BLK = 128
QUARTER = 16
CHUNKS = [(None, 0, 0), (None, 0, 1)] + [(p, d, h) for near in ((1, 3), (2,)) for h in range(2) for p in range(2) for d in near]
NUMBER = {chunk: q for q, chunk in enumerate(CHUNKS)}
SLOT = (0, 1, 3, 2)
RECEIVED, SENDING, LOCAL = 63, 15, 8


def split(value):
    high = value.astype(BF16)
    return high, (value - high.astype(F32)).astype(BF16)


def dot(a, b, precision=None):
    return jnp.dot(a, b, preferred_element_type=F32, precision=precision)


def aligned(start, size, unit):
    return pl.ds(pl.multiple_of(start, unit), size)


def kernel(
    tail, panel, rhs, block, out,
    tbuf, fwd, lbuf, lsplit, tt, cbuf, wrow, gfull, gsplit, rhs_in,
    r1, part, ring, psum, r3, xs, obuf,
    send_sem, recv_sem, local_sem,
):
    row, col = lax.axis_index("row"), lax.axis_index("col")
    x, core = row // 2, row % 2
    z, y = col // 4, col % 4

    def where(dx=0, dc=0, dz=0, dy=0):
        new_row = 2 * ((x + dx + 4) % 4) + (core + dc) % 2
        new_col = 4 * ((z + dz + 4) % 4) + (y + dy + 4) % 4
        return (new_row, new_col)

    def along(p, step):
        return where(dy=step) if p == 0 else where(dz=step)

    def across(p, step):
        return along(1 - p, step)

    place = (z, y)

    received, sending = {}, {}

    def copy(src, dst, target, group, sent):
        at, out_at = received.setdefault(group, len(received)), sending.setdefault(sent, len(sending))
        pltpu.make_async_remote_copy(
            src_ref=src,
            dst_ref=dst,
            send_sem=send_sem.at[out_at],
            recv_sem=recv_sem.at[at],
            device_id=target,
            device_id_type=pl.DeviceIdType.MESH,
        ).start()

    def arrived(group, ref):
        pltpu.make_async_copy(ref, ref, recv_sem.at[received[group]]).wait()

    def gone(sent, ref):
        pltpu.make_async_copy(ref, ref, send_sem.at[sending[sent]]).wait()

    local = []

    def bring(src, dst):
        made = pltpu.make_async_copy(src, dst, local_sem.at[len(local)])
        made.start()
        local.append(made)
        return made

    def piece(p, step, h):
        columns = pl.ds(h * BLK, BLK)
        if p == 0:
            return tail.at[:, (y + step) % 4, pl.ds(0, LEN[0]), columns]
        return tail.at[(z + step) % 4, :, pl.ds(LEN[0], LEN[1]), columns]

    def landing(p, d, h):
        return tbuf.at[p, SLOT[d], h, :, pl.ds(0, LEN[p]), :]

    partners = [where(dy=i) for i in (1, 2, 3)] + [where(dz=i) for i in (1, 2, 3)]
    partners += [where(dx=i, dc=j) for i in range(4) for j in range(2) if (i, j) != (0, 0)]
    barrier = pltpu.get_barrier_semaphore()
    for partner in partners:
        pl.semaphore_signal(barrier, inc=1, device_id=partner, device_id_type=pl.DeviceIdType.MESH)
    pl.semaphore_wait(barrier, len(partners))

    lanes = pl.ds(0, WIN // 2), pl.ds(WIN // 2, WIN // 2)
    for i in (1, 3, 2):
        copy(block, wrow.at[z, y], where(dy=i), "shards", "shards")

    def half(p, side):
        return pl.ds(0, 128) if side == 0 else pl.ds(128, LEN[p] - 128)

    def send_panel(p, step, side, group):
        src = pl.ds(p * PART + half(p, side).start, half(p, side).size)
        copy(panel.at[src, :], lbuf.at[p, place[p], half(p, side), :], across(p, step), group, ("panel", p))

    for p in (1, 0):
        send_panel(p, 1, 0, ("up", p))
        send_panel(p, 3, 1, ("down", p))
    own_block = bring(block, wrow.at[z, y])
    own_panel = [
        bring(panel.at[pl.ds(p * PART, LEN[p]), :], lbuf.at[p, place[p], pl.ds(0, LEN[p]), :]) for p in range(2)
    ]
    own_rhs = bring(rhs, rhs_in)
    own_tail = [bring(piece(p, 0, h), landing(p, 0, h)) for p in range(2) for h in range(2)]

    for i in range(4):
        lbuf[1, i, LEN[1] :, :] = jnp.zeros((PART - LEN[1], WIN), F32)
        for d in range(4):
            for h in range(2):
                tbuf[1, d, h, i, LEN[1] :, :] = jnp.zeros((PART - LEN[1], BLK), F32)

    own_block.wait()
    arrived("shards", wrow.at[0, pl.ds(0, 3)])
    for i in (1, 3, 2):
        copy(wrow.at[z], wrow.at[z], where(dz=i), "rows", "rows")
    for p in (1, 0):
        send_panel(p, 1, 1, ("second", p))
        send_panel(p, 3, 0, ("second", p))

    for p in (1, 0):
        for name, step, side in (("up", 1, 0), ("down", 3, 1)):
            at = lbuf.at[p, (place[p] - step + 4) % 4, half(p, side), :]
            arrived((name, p), at)
            copy(at, at, across(p, step), ("onward", p), ("panel", p))

    for p, d, h in CHUNKS[2:10]:
        copy(piece(p, d, h), landing(p, d, h), along(p, d), ("near", p, h), ("near", p))
    for h in range(2):
        for i in range(2):
            for p in range(2):
                side, columns = pl.ds(2 * i, 2), pl.ds(h * BLK, BLK)
                if p == 0:
                    src = tail.at[side, (y + 2) % 4, pl.ds(0, LEN[0]), columns]
                else:
                    src = tail.at[(z + 2) % 4, side, pl.ds(LEN[0], LEN[1]), columns]
                dst = fwd.at[p, h, i, :, pl.ds(0, LEN[p]), :]
                copy(src, dst, along(p, 1 + 2 * i), ("hop", p, h), ("hop", p))

    def relay(p, h):
        arrived(("hop", p, h), fwd.at[p, h, :, :, pl.ds(0, LEN[p]), :])
        for i in range(2):
            src = fwd.at[p, h, i, :, pl.ds(0, LEN[p]), :]
            dst = tbuf.at[p, SLOT[2], h, pl.ds(2 * i, 2), pl.ds(0, LEN[p]), :]
            copy(src, dst, along(p, 1 + 2 * i), ("far", p, h), ("far", p))

    arrived("rows", wrow.at[pl.ds(0, 3)])

    rows = lax.broadcasted_iota(jnp.int32, (BLK, BLK), 0)
    cols = lax.broadcasted_iota(jnp.int32, (BLK, BLK), 1)
    eye = jnp.where(rows == cols, 1.0, 0.0).astype(F32)
    own_cols = aligned(row * BLK, BLK, BLK)
    diagonal = wrow[:, :, :, own_cols].reshape(BLK, BLK)
    on_diag = jnp.where(rows == cols, diagonal, 0.0)
    diag_rows = jnp.sum(on_diag, axis=1, keepdims=True)
    diag_cols = jnp.sum(on_diag, axis=0, keepdims=True)
    lower = jnp.where(rows > cols, diagonal, 0.0) / diag_rows
    inverse, power = eye - lower, dot(lower, lower, HIGHEST)
    for _ in range(6):
        both = dot(jnp.concatenate([inverse, power], axis=0), power, HIGHEST)
        inverse, power = inverse + both[:BLK], both[BLK:]
    inverse = inverse / diag_cols
    gfull[row] = dot(inverse, wrow[...].reshape(BLK, WIN), HIGHEST)
    gfull[row, :, own_cols] = inverse
    for i in (1, 3, 2):
        copy(gfull.at[row], gfull.at[row], where(dx=i), "over_x", "blocks")
    copy(gfull.at[row], gfull.at[row], where(dc=1), "to_other", "blocks")

    def split_panel(p, slot):
        @pl.loop(0, 2)
        def _(step):
            high, low = split(lbuf[p, slot, aligned(step * BLK, BLK, BLK), :])
            lsplit[p, aligned(slot * PART + step * BLK, BLK, BLK), :] = low
            lsplit[p, aligned(DEEP + slot * PART + step * BLK, BLK, BLK), :] = high

    def turn(p, i, d, h, slots):
        @pl.loop(*slots)
        def _(step):
            high, low = split(tbuf[p, SLOT[d], h, step].T)
            tt[p, pl.ds(i * BLK, BLK), aligned(step * PART, PART, PART)] = high
            tt[p, pl.ds(i * BLK, BLK), aligned(DEEP + step * PART, PART, PART)] = low

    def add_own(p, slot):
        high_at, low_at = aligned(slot * PART, PART, PART), aligned(DEEP + slot * PART, PART, PART)

        @pl.loop(0, 4)
        def _(step):
            at = aligned(step * 256, 256, 256)
            value = dot(tt[p, :, low_at], lsplit[p, low_at, at]) + dot(tt[p, :, high_at], lsplit[p, high_at, at])
            value += dot(tt[p, :, high_at], lsplit[p, low_at, at])
            cbuf[0, :, at] += value[:BLK]
            cbuf[1, :, at] += value[BLK:]

    for made in own_panel + own_tail:
        made.wait()
    own_rhs.wait()
    turned = rhs_in[...].T
    for h in range(2):
        cbuf[h] = jnp.zeros((BLK, WIN), F32)
        cbuf[h, :, own_cols] = -turned[h * BLK : (h + 1) * BLK]
    for p in range(2):
        split_panel(p, place[p])
        for h in range(2):
            turn(p, h, 0, h, (0, 4))
    for p in (1, 0):
        arrived(("second", p), lbuf.at[p, 0, pl.ds(0, LEN[p]), :])
        split_panel(p, (place[p] + 3) % 4)
        split_panel(p, (place[p] + 1) % 4)

        @pl.loop(0, 3)
        def _(i):
            add_own(p, (place[p] + 3 + i) % 4)

    for p in (1, 0):
        arrived(("onward", p), lbuf.at[p, 0, pl.ds(0, LEN[p]), :])
        split_panel(p, (place[p] + 2) % 4)
        add_own(p, (place[p] + 2) % 4)

    keep, give = aligned(core * 64, 64, 64), aligned((1 - core) * 64, 64, 64)

    def to_pair(q, n, s):
        at = pl.ds(q, n)
        copy(cbuf.at[at, give, lanes[s]], r1.at[at, :, lanes[s]], where(dc=1), ("pair", q, s), "pair")

    def to_ring(q, n, s):
        at = pl.ds(q, n)
        arrived(("pair", q, s), r1.at[at, :, lanes[s]])
        value = cbuf[at, keep, lanes[s]] + r1[at, :, lanes[s]]
        part[at, :, :, lanes[s]] = value.reshape(n, 4, QUARTER, WIN // 2)
        for i in (2, 1, 3):
            src, dst = part.at[at, (x + i) % 4, :, lanes[s]], ring.at[at, i - 1, :, lanes[s]]
            copy(src, dst, where(dx=i), ("ring", q, s), "ring")

    def from_ring(q, n, s):
        arrived(("ring", q, s), ring.at[pl.ds(q, n), :, :, lanes[s]])
        at = lanes[s]
        for k in range(q, q + n):
            psum[k, :, at] = part[k, x, :, at] + ring[k, 0, :, at] + ring[k, 1, :, at] + ring[k, 2, :, at]

    def to_owner(q, at=pl.ds(0, WIN)):
        p, d, _ = CHUNKS[q]
        copy(psum.at[q, :, at], r3.at[q - 2, :, at], along(p, -d), ("owner", d == 2), "owner")

    def near_product(p, h, s):
        if s:
            arrived(("near", p, h), tbuf.at[p, pl.ds(1, 2), h, :, pl.ds(0, LEN[p]), :])
            for i, d in enumerate((1, 3)):
                turn(p, i, d, h, (0, 4))
        q = NUMBER[p, 1, h]

        @pl.loop(2 * s, 2 * s + 2)
        def _(step):
            at = aligned(step * 256, 256, 256)
            value = dot(tt[p], lsplit[p, :, at]) + dot(tt[p, :, :DEEP], lsplit[p, DEEP:, at])
            for i in range(2):
                cbuf[q + i, :, at] = value[i * BLK : (i + 1) * BLK]

        to_pair(q, 2, s)

    def far_product(p, h, s):
        if s:
            arrived(("far", p, h), landing(p, 2, h))

            @pl.loop(0, 4)
            def _(step):
                high, low = split(tbuf[p, SLOT[2], h, step].T)
                tt[p, pl.ds(0, BLK), aligned(step * PART, PART, PART)] = high
                tt[p, pl.ds(BLK, BLK), aligned(step * PART, PART, PART)] = low

        q = NUMBER[p, 2, h]

        @pl.loop(2 * s, 2 * s + 2)
        def _(step):
            at = aligned(step * 256, 256, 256)
            both = dot(tt[p, :, :DEEP], lsplit[p, DEEP:, at])
            cbuf[q, :, at] = both[:BLK] + both[BLK:] + dot(tt[p, :BLK, :DEEP], lsplit[p, :DEEP, at])

        to_pair(q, 1, s)

    to_pair(0, 2, 1)
    to_pair(0, 2, 0)
    to_ring(0, 2, 1)
    to_ring(0, 2, 0)
    near_product(0, 0, 1)
    near_product(0, 0, 0)
    to_ring(2, 2, 1)
    near_product(1, 0, 1)
    to_ring(2, 2, 0)
    near_product(1, 0, 0)
    to_ring(4, 2, 1)
    arrived("over_x", gfull.at[pl.ds(0, 3)])
    for i in (1, 3, 2):
        slot = 2 * ((x - i + 4) % 4) + core
        copy(gfull.at[slot], gfull.at[slot], where(dc=1), "to_other", "blocks")
    to_ring(4, 2, 0)
    from_ring(0, 2, 1)
    from_ring(0, 2, 0)
    near_product(0, 1, 1)
    near_product(0, 1, 0)
    to_ring(6, 2, 1)
    near_product(1, 1, 1)
    to_ring(6, 2, 0)
    near_product(1, 1, 0)
    to_ring(8, 2, 1)
    relay(0, 0)
    relay(1, 0)
    to_ring(8, 2, 0)
    arrived("to_other", gfull.at[pl.ds(0, 4)])

    @pl.loop(0, 8)
    def _(step):
        high, low = split(gfull[step])
        gsplit[0, step] = high
        gsplit[1, step] = low

    relay(0, 1)
    relay(1, 1)
    for q in (2, 4):
        for s in (1, 0):
            from_ring(q, 2, s)
    far_product(0, 0, 1)
    far_product(0, 0, 0)
    to_ring(10, 1, 1)
    to_ring(10, 1, 0)
    far_product(1, 0, 1)
    far_product(1, 0, 0)
    to_ring(11, 1, 1)
    far_product(0, 1, 1)
    to_ring(11, 1, 0)
    far_product(0, 1, 0)
    to_ring(12, 1, 1)
    far_product(1, 1, 1)
    to_ring(12, 1, 0)
    far_product(1, 1, 0)
    to_ring(13, 1, 1)
    for q in (6, 8):
        for s in (1, 0):
            from_ring(q, 2, s)
    for q in (2, 3, 6, 7):
        to_owner(q)
    to_ring(13, 1, 0)
    for q in (4, 5, 8, 9):
        to_owner(q)
    for q in (10, 11, 12, 13):
        for s in (1, 0):
            from_ring(q, 1, s)
            to_owner(q, lanes[s])
    totals = [psum[0], psum[1]]
    for far, distances, count in ((False, (1, 3), 8), (True, (2,), 4)):
        arrived(("owner", far), r3.at[pl.ds(8 * far, count)])
        for h in range(2):
            for d in distances:
                for p in range(2):
                    totals[h] += r3[NUMBER[p, d, h] - 2]

    own = aligned(core * 64 + x * QUARTER, QUARTER, QUARTER)
    left = -jnp.concatenate(totals, axis=0)
    for j in range(7, -1, -1):
        high, low = split(left[:, j * BLK : (j + 1) * BLK])
        width = (j + 1) * BLK
        both = dot(jnp.concatenate([high, low], axis=0), gsplit[0, j, :, :width])
        step = both[:32] + both[32:] + dot(high, gsplit[1, j, :, :width])
        xs[j] = step[:, j * BLK :].reshape(2, QUARTER, BLK)

        @pl.when(row != j)
        def _():
            copy(xs.at[j], obuf.at[:, own, :], (j, col), "spread", "spread")

        if j:
            left = left[:, : j * BLK] - step[:, : j * BLK]

    obuf[:, own, :] = xs[row]
    arrived("spread", xs.at[pl.ds(0, 7)])
    out[...] = obuf[...].reshape(COLS, BLK).T
    gone("shards", wrow.at[0, pl.ds(0, 3)])
    gone("rows", wrow.at[pl.ds(0, 3)])
    gone("blocks", gfull.at[pl.ds(0, 7)])
    for p in range(2):
        gone(("panel", p), lbuf.at[p, pl.ds(0, 3), pl.ds(0, LEN[p]), :])
        gone(("near", p), tbuf.at[p, pl.ds(1, 2), :, :, pl.ds(0, LEN[p]), :])
        gone(("hop", p), fwd.at[p, :, :, :, pl.ds(0, LEN[p]), :])
        gone(("far", p), tbuf.at[p, SLOT[2], :, :, pl.ds(0, LEN[p]), :])
    gone("pair", r1)
    gone("ring", ring)
    gone("owner", r3)
    gone("spread", xs.at[pl.ds(0, 7)])
    assert len(received) == RECEIVED and len(sending) == SENDING


def per_device(tail_vectors, lower_panel, window_rhs, window_block):
    anywhere = pl.BlockSpec(memory_space=pl.ANY)
    count = len(CHUNKS)
    return pl.pallas_call(
        kernel,
        name="window_solve",
        out_shape=jax.ShapeDtypeStruct((BLK, COLS), F32),
        in_specs=[anywhere] * 4,
        out_specs=pl.BlockSpec(memory_space=pltpu.VMEM),
        scratch_shapes=[
            pltpu.VMEM((2, 4, 2, 4, PART, BLK), F32),
            pltpu.VMEM((2, 2, 2, 2, PART, BLK), F32),
            pltpu.VMEM((2, 4, PART, WIN), F32),
            pltpu.VMEM((2, 2 * DEEP, WIN), BF16),
            pltpu.VMEM((2, COLS, 2 * DEEP), BF16),
            pltpu.VMEM((count, BLK, WIN), F32),
            pltpu.VMEM((4, 4, 8, WIN), F32),
            pltpu.VMEM((8, BLK, WIN), F32),
            pltpu.VMEM((2, 8, BLK, WIN), BF16),
            pltpu.VMEM((BLK, COLS), F32),
            pltpu.VMEM((count, 64, WIN), F32),
            pltpu.VMEM((count, 4, QUARTER, WIN), F32),
            pltpu.VMEM((count, 3, QUARTER, WIN), F32),
            pltpu.VMEM((count, QUARTER, WIN), F32),
            pltpu.VMEM((count - 2, QUARTER, WIN), F32),
            pltpu.VMEM((8, 2, QUARTER, BLK), F32),
            pltpu.VMEM((2, BLK, BLK), F32),
            pltpu.SemaphoreType.DMA((SENDING,)),
            pltpu.SemaphoreType.DMA((RECEIVED,)),
            pltpu.SemaphoreType.DMA((LOCAL,)),
        ],
        compiler_params=pltpu.CompilerParams(
            collective_id=0, has_side_effects=True, vmem_limit_bytes=62 * 1024 * 1024
        ),
    )(tail_vectors.reshape(4, 4, SEG, COLS), lower_panel, window_rhs, window_block)


def solution(mesh):
    in_specs = (P("row", "col"), P(("row", "col"), None), P("row", "col"), P(("row", "col"), None))
    return jax.shard_map(
        per_device, mesh=mesh, in_specs=in_specs, out_specs=P("row", "col"), check_vma=False
    )
```
